128 devices in a mesh: dp: 4 (over x), section: 2 (over core), tensor: 16 (over z, y).
Axes of the slice: x: 4, y: 4, z: 4, core: 2. Of those that a mesh axis runs over, the one named last changes fastest.
Arguments:
- in_delta: bfloat16 [8, 1024, 4096], P(None, ('dp', 'tensor')), may hold values from -12 to 12
- weight: bfloat16 [2, 4096, 4096], P('section', 'tensor'), may hold values from -0.09375 to 0.09375
- cache_codes: int32 [2, 2, 8, 1024, 4096], P('section', None, None, ('dp', 'tensor')), may hold values from -7 to 7, as said below
- cache_scales: float32 [2, 2, 8, 4, 32], P('section', None, None, 'dp'), may hold values from 0.2 to 6, as said below
- cotangent: bfloat16 [8, 1024, 4096], P(None, ('dp', 'tensor')), may hold values from -16 to 16
Outputs:
- out_deltas: bfloat16 [2, 8, 1024, 4096], P('section', None, ('dp', 'tensor'))
- grad_in: bfloat16 [2, 8, 1024, 4096], P('section', None, ('dp', 'tensor'))
- weight_grad: float32 [2, 4096, 4096], P('section', 'tensor', 'dp')
The draws below stay inside these ranges and needn't reach their ends.
Inputs may be any that keep to these rules, and one draw needn't show every extreme that they name: cache_codes[s, 1] equals cache_codes[s + 1, 0]: the buffer of a boundary between two segments is held by both. cache_scales[s, 1] equals cache_scales[s + 1, 0].
All inputs are finite; a program needn't handle non-finite values. Where the reference program divides by a largest or mean magnitude, that divisor is 1e-20 or more.
Results may differ from the reference program's by a relative error of at most 0.013.
Values may be sent and summed in bfloat16 or wider, within the bound.
No kernel may reach another device: no remote copies, remote signals or barrier semaphores. Data moves between devices by JAX's collectives and lax.ppermute only.
A program may use at most 128 MiB of HBM per device.

```python
import jax
import jax.numpy as jnp
from jax import lax

D = 4096
BLOCK = 128
MBT = 256
MICRO = 8
SECTIONS = 2
BLOCKS = 32
TOKENS = 1024
N_DP = 4
N_TENSOR = 16


def boundary_codes(key):
    sub_key = jax.random.fold_in(key, 17)
    return jax.random.randint(sub_key, (SECTIONS + 1, MICRO, TOKENS, D), -7, 8, dtype=jnp.int32)


def draw_cache_codes(key, part):
    stacked = boundary_codes(key)
    return jnp.stack([stacked[:-1], stacked[1:]], axis=1)


def draw_cache_scales(key, part):
    sub_key = jax.random.fold_in(key, 29)
    shape_all = (SECTIONS + 1, MICRO, N_DP, BLOCKS)
    logs = jax.random.uniform(sub_key, shape_all, jnp.float32, jnp.log(0.5), jnp.log(4.0))
    stacked = jnp.exp(logs)
    return jnp.stack([stacked[:-1], stacked[1:]], axis=1)


def draw_in_delta(key, part):
    first_key, second_key = jax.random.split(jax.random.fold_in(key, 41), 2)
    shape_all = (MICRO, TOKENS, D)
    row_factor = jnp.exp(jax.random.uniform(second_key, (MICRO, TOKENS, 1), jnp.float32, jnp.log(0.3), jnp.log(3.0)))
    values = jax.random.normal(first_key, shape_all, jnp.float32) * row_factor
    return jnp.clip(values, -12.0, 12.0).astype(jnp.bfloat16)


def with_spikes(array, rng, source, target, blocks, factor):
    owner, partner = [(jnp.arange(array.shape[axis_at]) // (array.shape[axis_at] // blocks)).reshape([-1 if axis == axis_at else 1 for axis in range(array.ndim)]) for axis_at in (source, target)]
    chosen = jax.random.permutation(rng, blocks)[partner]
    strong = (owner == chosen) | (owner == (partner + blocks // 2) % blocks)
    return jnp.where(strong, factor * array, array)


def block_scale(rng, dims, pieces, smallest, high):
    loudness, own = 1.0, jax.random.fold_in(rng, 6)
    for axis_at, shards_of in pieces:
        steps = jnp.exp(jax.random.uniform(jax.random.fold_in(own, axis_at), (shards_of,), jnp.float32, smallest / len(pieces), high / len(pieces)))
        loudness = loudness * jnp.repeat(steps, dims[axis_at] // shards_of).reshape([-1 if axis == axis_at else 1 for axis in range(len(dims))])
    return loudness


def bell_draw(own_key, extent, scale, bound, pieces=(), held_as=jnp.bfloat16):
    values = scale * jax.random.normal(own_key, extent, jnp.float32)
    if pieces:
        values = values * block_scale(own_key, extent, pieces, -0.22, 0.18)
    return jnp.clip(values, -bound, bound).astype(held_as)


def gaussian_with(stream_key, shape, scale, reach, cuts, heavy, kind=jnp.bfloat16):
    entries = scale * jax.random.normal(stream_key, shape, jnp.float32)
    if cuts:
        entries = entries * block_scale(stream_key, shape, cuts, -0.22, 0.18)
    return jnp.clip(with_spikes(entries, jax.random.fold_in(stream_key, 3), *heavy), -reach, reach).astype(kind)


def setup_inputs(seed: int = 0) -> dict:
    splits = jax.random.split(jax.random.key(seed), 6)
    in_delta = draw_in_delta(jax.random.fold_in(splits[5], 71), 0)
    weight = bell_draw(splits[1], (SECTIONS, D, D), D ** -0.5, 0.09375, ((0, 2), (1, 16)))
    cache_codes = draw_cache_codes(jax.random.fold_in(splits[5], 71), 0)
    cache_scales = draw_cache_scales(jax.random.fold_in(splits[5], 71), 0)
    cotangent = gaussian_with(splits[4], (MICRO, TOKENS, D), 1.0, 16.0, ((1, 64),), (1, 2, 64, 4.0))
    return dict(in_delta=in_delta, weight=weight, cache_codes=cache_codes, cache_scales=cache_scales, cotangent=cotangent)


code_levels = 7.0
softness = 0.8
two_pi = 6.283185307179586
epsilon = 1e-06

def dequantize(stored_codes, scales_all):
    blocked = stored_codes.astype(jnp.float32).reshape(MICRO, N_DP, MBT, BLOCKS, BLOCK)
    return (blocked * scales_all[:, :, None, :, None] / code_levels).reshape(MICRO, TOKENS, D)

def quantize(boundary_delta):
    blocked = boundary_delta.reshape(MICRO, N_DP, MBT, BLOCKS, BLOCK)
    spread = (lax.optimization_barrier(jnp.max(jnp.abs(blocked), axis=(2, 4))) + epsilon)[:, :, None, :, None]
    level_value = code_levels * blocked / spread
    smooth = level_value - softness * jnp.sin(two_pi * level_value) / two_pi
    return (smooth * spread / code_levels).astype(jnp.bfloat16).reshape(MICRO, TOKENS, D)

def grouped_product(normed, weight_now):
    flat = normed.reshape(-1, D)
    group_width = D // N_TENSOR
    total = jnp.zeros((flat.shape[0], D), jnp.float32)
    for group in range(N_TENSOR):
        piece = jnp.dot(flat[:, group * group_width:(group + 1) * group_width], weight_now[group * group_width:(group + 1) * group_width], preferred_element_type=jnp.float32)
        total = total + lax.optimization_barrier(piece.astype(jnp.bfloat16)).astype(jnp.float32)
    return total.reshape(MICRO, TOKENS, D)

def reference(in_delta, weight, cache_codes, cache_scales, cotangent):
    incoming = in_delta
    saved_states = []
    sent_all = []
    for segment_now in range(SECTIONS):
        hidden = dequantize(cache_codes[segment_now, 0], cache_scales[segment_now, 0]) + incoming.astype(jnp.float32)
        scaling = lax.rsqrt(lax.optimization_barrier(jnp.mean(hidden * hidden, axis=-1, keepdims=True)) + epsilon)
        normed = (hidden * scaling).astype(jnp.bfloat16)
        branch = grouped_product(normed, weight[segment_now])
        boundary_delta = hidden + branch - dequantize(cache_codes[segment_now, 1], cache_scales[segment_now, 1])
        incoming = quantize(boundary_delta)
        saved_states.append((hidden, scaling, normed))
        sent_all.append(incoming)
    upstream = cotangent
    grads_in = [None] * SECTIONS
    weight_grads = [None] * SECTIONS
    for segment_now in range(SECTIONS - 1, -1, -1):
        hidden, scaling, normed = saved_states[segment_now]
        grad_raw = jnp.dot(upstream.reshape(-1, D), weight[segment_now].T, preferred_element_type=jnp.float32).reshape(MICRO, TOKENS, D)
        grad_normed = lax.optimization_barrier(grad_raw.astype(jnp.bfloat16)).astype(jnp.float32)
        normed_rep = normed.reshape(MICRO, N_DP, MBT, D)
        upstream_rep = upstream.reshape(MICRO, N_DP, MBT, D)
        total = jnp.zeros((D, D), jnp.float32)
        for replica in range(N_DP):
            partial_sum = jnp.dot(normed_rep[:, replica].reshape(-1, D).T, upstream_rep[:, replica].reshape(-1, D), preferred_element_type=jnp.float32)
            total = total + lax.optimization_barrier(partial_sum.astype(jnp.bfloat16)).astype(jnp.float32)
        unrounded = hidden * scaling
        grad_hidden = upstream.astype(jnp.float32) + scaling * (grad_normed - unrounded * lax.optimization_barrier(jnp.mean(grad_normed * unrounded, axis=-1, keepdims=True)))
        upstream = grad_hidden.astype(jnp.bfloat16)
        grads_in[segment_now] = upstream
        weight_grads[segment_now] = total
    return (jnp.stack(sent_all), jnp.stack(grads_in), jnp.stack(weight_grads))
```

```python
import jax
import jax.numpy as jnp
from jax import lax
from jax.sharding import Mesh
from jax.sharding import PartitionSpec as P


TENSOR = ("tensor_0", "tensor_1")
CHIP = ("section", "tensor_0", "tensor_1")
DP_TENSOR = ("dp", "tensor_0", "tensor_1")
SIDE = 4
CHUNKS = 1

code_levels = 7.0
softness = 0.8
two_pi = 6.283185307179586
epsilon = 1e-06

SINE = (25.13274118, -64.8358279, 67.07681018, -38.49815464, 14.06107271, -3.181409966)


def shift(value, phase, along, steps):
    pairs = []
    for s in range(2):
        on_z = ((s + phase) % 2 == 0) == (along == "rows")
        for z in range(SIDE):
            for y in range(SIDE):
                to_z = (z + steps) % SIDE if on_z else z
                to_y = y if on_z else (y + steps) % SIDE
                pairs.append(((s * SIDE + z) * SIDE + y, (s * SIDE + to_z) * SIDE + to_y))
    return lax.ppermute(value, CHIP, pairs)


def ring(value, axis, steps):
    return lax.ppermute(value, axis, [(i, (i + steps) % SIDE) for i in range(SIDE)])


def pick(stacked, at):
    return lax.dynamic_index_in_dim(stacked, at % SIDE, 0, keepdims=False)


def placed(pieces, positions):
    buffer = jnp.zeros((SIDE, *pieces[0].shape), pieces[0].dtype)
    for piece, at in zip(pieces, positions):
        buffer = lax.dynamic_update_index_in_dim(buffer, piece, at % SIDE, 0)
    return buffer


def blocks_of(rows):
    width = rows.shape[-1] // SIDE
    return jnp.stack([rows[..., i * width : (i + 1) * width] for i in range(SIDE)])


def joined(blocks):
    return jnp.concatenate([blocks[i] for i in range(SIDE)], axis=-1)


def widened(scales, width):
    count = scales.shape[-1]
    wide = jnp.broadcast_to(scales[..., None], (*scales.shape, width // count))
    return wide.reshape(scales.shape[0], 1, width)


def dequantize(codes, scales):
    return codes.astype(jnp.float32) * widened(scales / code_levels, codes.shape[-1])


def soft_codes(boundary_delta, spread):
    width = boundary_delta.shape[-1]
    level = boundary_delta * widened(code_levels / spread, width)
    part = level - jnp.round(level)
    square = part * part
    poly = jnp.full_like(square, SINE[-1])
    for coefficient in SINE[-2::-1]:
        poly = poly * square + coefficient
    sine = part * (0.25 - square) * poly
    smooth = level - (softness / two_pi) * sine
    return (smooth * widened(spread / code_levels, width)).astype(jnp.bfloat16)


def largest(boundary_delta, block_count):
    columns = jnp.max(jnp.abs(boundary_delta), axis=1)
    peak = jnp.max(columns.reshape(columns.shape[0], block_count, -1), axis=-1)
    for axis in ("tensor_0", "tensor_1"):
        arrived = [ring(peak, axis, k) for k in (1, 2, 3)]
        for other in arrived:
            peak = jnp.maximum(peak, other)
    return peak + epsilon


def inverse_rms(hidden):
    return lax.rsqrt(jnp.mean(hidden * hidden, axis=-1, keepdims=True) + epsilon)


def through_norm(upstream, hidden, scaling, grad_normed):
    unrounded = hidden * scaling
    grad = grad_normed.astype(jnp.float32)
    mean = jnp.mean(grad * unrounded, axis=-1, keepdims=True)
    return (upstream.astype(jnp.float32) + scaling * (grad - unrounded * mean)).astype(
        jnp.bfloat16
    )


def dot(a, b, dims):
    return lax.dot_general(a, b, (dims, ((), ())), preferred_element_type=jnp.float32)


def local(in_delta, weight, cache_codes, cache_scales, cotangent):
    s = lax.axis_index("section")
    z = lax.axis_index("tensor_0")
    y = lax.axis_index("tensor_1")
    x = lax.axis_index("dp")
    first = s == 0
    micro_count, local_rows, width = in_delta.shape
    span = width // SIDE
    block_count = cache_scales.shape[-1]
    scales = cache_scales[0, :, :, 0, :]
    codes = cache_codes[0]

    columns = blocks_of(weight[0])
    pieces = [pick(columns, y)] + [ring(pick(columns, y + k), "tensor_1", k) for k in (1, 2, 3)]
    block = placed(pieces, [y - k for k in range(SIDE)]).reshape(span, span)
    turned = block.T
    sides = (jnp.where(first, block, turned), jnp.where(first, turned, block))

    def at(phase):
        on_z = first if phase == 0 else jnp.logical_not(first)
        return jnp.where(on_z, z, y), jnp.where(on_z, y, z)

    def spread_out(tokens, phase):
        a, _ = at(phase)
        cut = blocks_of(tokens.reshape(-1, width))
        mine = jnp.stack(
            [pick(cut, a)] + [shift(pick(cut, a + k), phase, "rows", k) for k in (1, 2, 3)]
        )
        return [mine] + [shift(mine, phase, "columns", j) for j in (1, 2, 3)]

    def multiplied(groups, phase):
        _, b = at(phase)
        sent = {}
        for k in (2, 1, 3, 0):
            rows = jnp.concatenate([group[k] for group in groups])
            product = dot(rows, sides[phase], ((1,), (0,))).astype(jnp.bfloat16)
            sent[k] = product if k == 0 else shift(product, phase, "rows", -k)
        total = sum(sent[k].astype(jnp.float32) for k in range(SIDE)).astype(jnp.bfloat16)
        total = total.reshape(SIDE, -1, span)
        home = [total[0]] + [shift(total[j], phase, "columns", -j) for j in (1, 2, 3)]
        result = joined(placed(home, [b + j for j in range(SIDE)]))
        return result.reshape(-1, local_rows, width)

    def swapped(value, source):
        return lax.ppermute(value, "section", [(source, 1 - source)])

    per_chunk = micro_count // CHUNKS
    outs, grads, lefts, rights = [], [], [], []
    for chunk in range(CHUNKS):
        now = slice(chunk * per_chunk, (chunk + 1) * per_chunk)
        near, far = codes[0, now], codes[1, now]
        near_scales, far_scales = scales[0, now], scales[1, now]
        delta_in, cot = in_delta[now], cotangent[now]
        hidden = dequantize(near, near_scales) + delta_in.astype(jnp.float32)
        scaling = inverse_rms(hidden)
        normed = (hidden * scaling).astype(jnp.bfloat16)
        groups = spread_out(jnp.where(first, normed, cot), 0)
        result = multiplied(groups, 0)
        early = swapped(result, 1)
        boundary = hidden + result.astype(jnp.float32) - dequantize(far, far_scales)
        out_here = soft_codes(boundary, largest(boundary, block_count))
        out_first = jnp.where(first, out_here, swapped(out_here, 0))
        grad_raw = jnp.where(first, early, result)
        middle = dequantize(jnp.where(first, far, near), jnp.where(first, far_scales, near_scales))
        hidden_last = middle + out_first.astype(jnp.float32)
        scaling_last = inverse_rms(hidden_last)
        normed_last = (hidden_last * scaling_last).astype(jnp.bfloat16)
        grad_last = through_norm(cot, hidden_last, scaling_last, grad_raw)
        groups_next = spread_out(jnp.where(first, grad_last, normed_last), 1)
        result_next = multiplied(groups_next, 1)
        boundary_next = hidden_last + result_next.astype(jnp.float32) - dequantize(far, far_scales)
        out_next = soft_codes(boundary_next, largest(boundary_next, block_count))
        outs.append(jnp.where(first, out_first, out_next))
        grad_first = through_norm(grad_last, hidden, scaling, result_next)
        grads.append(jnp.where(first, grad_first, grad_last))
        lefts.append(jnp.concatenate([group[k] for k in range(SIDE) for group in groups]))
        rights.append(jnp.concatenate([group.reshape(-1, span) for group in groups_next]))

    left, right = jnp.concatenate(lefts), jnp.concatenate(rights)
    inputs, ups = jnp.where(first, left, right), jnp.where(first, right, left)
    partial = dot(inputs, ups, ((0,), (0,))).astype(jnp.bfloat16)
    quarters = blocks_of(partial)
    summed = sum(
        [pick(quarters, x).astype(jnp.float32)]
        + [ring(pick(quarters, x + k), "dp", k).astype(jnp.float32) for k in (1, 2, 3)]
    ).astype(jnp.bfloat16)
    rows = summed.reshape(SIDE, -1, span // SIDE)
    owned = [pick(rows, y)] + [ring(pick(rows, y + k), "tensor_1", k) for k in (1, 2, 3)]
    owned = placed(owned, [y - k for k in range(SIDE)])
    final = [pick(owned, x)] + [ring(pick(owned, x + k), "dp", k) for k in (1, 2, 3)]
    weight_grad = joined(placed(final, [x - k for k in range(SIDE)])).astype(jnp.float32)
    return (jnp.concatenate(outs)[None], jnp.concatenate(grads)[None], weight_grad[None])


def solution(mesh):
    finer = Mesh(
        mesh.devices.reshape(mesh.shape["dp"], mesh.shape["section"], SIDE, SIDE),
        ("dp", "section", "tensor_0", "tensor_1"),
    )
    return jax.shard_map(
        local,
        mesh=finer,
        in_specs=(
            P(None, DP_TENSOR, None),
            P("section", TENSOR, None),
            P("section", None, None, DP_TENSOR, None),
            P("section", None, None, "dp", None),
            P(None, DP_TENSOR, None),
        ),
        out_specs=(
            P("section", None, DP_TENSOR, None),
            P("section", None, DP_TENSOR, None),
            P("section", TENSOR, "dp"),
        ),
        check_vma=False,
    )
```

```python
import functools

import jax
import jax.numpy as jnp
from jax import lax
from jax.experimental import pallas as pl
from jax.experimental.pallas import tpu as pltpu
from jax.sharding import Mesh
from jax.sharding import PartitionSpec as P


TENSOR = ("tensor_0", "tensor_1")
CHIP = ("section", "tensor_0", "tensor_1")
DP_TENSOR = ("dp", "tensor_0", "tensor_1")
SIDE = 4
BLOCK = 128
PER = 8
STEPS = 2
VMEM_LIMIT = 24 * 1024 * 1024

code_levels = 7.0
softness = 0.8
two_pi = 6.283185307179586
epsilon = 1e-06

SINE = (25.13274118, -64.8358279, 67.07681018, -38.49815464, 14.06107271, -3.181409966)


def on_z(s, phase, along):
    return ((s + phase) % 2 == 0) == (along == "rows")


def position(s, z, y):
    return (s * SIDE + z) * SIDE + y


def shift(value, phase, along, steps):
    pairs = []
    for s in range(2):
        for z in range(SIDE):
            for y in range(SIDE):
                if on_z(s, phase, along):
                    target = position(s, (z + steps) % SIDE, y)
                else:
                    target = position(s, z, (y + steps) % SIDE)
                pairs.append((position(s, z, y), target))
    return lax.ppermute(value, CHIP, pairs)


def ring(value, axis, steps):
    return lax.ppermute(value, axis, [(i, (i + steps) % SIDE) for i in range(SIDE)])


def crossed_over(value):
    return lax.ppermute(value, "section", [(0, 1), (1, 0)])


def to_owner(value, k):
    pairs = []
    for x in range(SIDE):
        for s in range(2):
            for y in range(SIDE):
                row = (x + k) % SIDE if s == 0 else x
                pairs.append(((x * 2 + s) * SIDE + y, (y * 2 + s) * SIDE + row))
    return lax.ppermute(value, ("dp", "section", "tensor_1"), pairs)


def lanes(block):
    return slice(block * BLOCK, (block + 1) * BLOCK)


def f32(value):
    return value.astype(jnp.float32)


def call(body, ids, grid, inputs, in_specs, shapes, out_specs, scratch=(), flops=0, aliases=None):
    cost = pl.CostEstimate(flops=flops or 20_000_000, bytes_accessed=8_000_000, transcendentals=0)
    return pl.pallas_call(
        body,
        grid_spec=pltpu.PrefetchScalarGridSpec(
            num_scalar_prefetch=1,
            grid=grid,
            in_specs=in_specs,
            out_specs=out_specs,
            scratch_shapes=scratch,
        ),
        out_shape=shapes,
        cost_estimate=cost,
        compiler_params=pltpu.CompilerParams(vmem_limit_bytes=VMEM_LIMIT),
        input_output_aliases=aliases or {},
    )(ids, *inputs)


def root_mean(squares, width):
    return lax.rsqrt(jnp.sum(squares, axis=-1, keepdims=True) * (1.0 / width) + epsilon)


def column(place, steps, inner):
    n = lax.rem(place + steps + SIDE, SIDE)
    return pl.ds(pl.multiple_of(n * PER * BLOCK + inner * BLOCK, BLOCK), BLOCK)


def scale_at(scales, slot, micro, place, steps, inner):
    n = lax.rem(place + steps + SIDE, SIDE)
    return scales[slot, micro, n * PER + inner] / code_levels


def each_micro(count, step):
    lax.fori_loop(0, count, lambda m, _: (step(m), None)[1], None)


def first_body(ids, scales, near, arriving, cot, *refs):
    outs, hidden = refs[:SIDE], refs[SIDE]
    count, rows, width = arriving.shape
    start = pl.program_id(0) * count

    @pl.when(ids[0] == 0)
    def _():
        def step(m):
            i = start + m
            at_rows = pl.ds(pl.multiple_of(m * rows, rows), rows)
            squares = jnp.zeros((rows, BLOCK), jnp.float32)
            for block in range(width // BLOCK):
                at = lanes(block)
                value = f32(near[0, m, :, at]) * (scales[0, i, block] / code_levels) + f32(
                    arriving[m, :, at]
                )
                hidden[:, at] = value
                squares = squares + value * value
            inverse = root_mean(squares, width)
            for k in range(SIDE):
                for inner in range(PER):
                    normed = hidden[:, column(ids[1], k, inner)] * inverse
                    outs[k][at_rows, lanes(inner)] = normed.astype(jnp.bfloat16)

        each_micro(count, step)

    @pl.when(ids[0] != 0)
    def _():
        def step(m):
            at_rows = pl.ds(pl.multiple_of(m * rows, rows), rows)
            for k in range(SIDE):
                for inner in range(PER):
                    outs[k][at_rows, lanes(inner)] = cot[m, :, column(ids[1], k, inner)]

        each_micro(count, step)


def first_side_body(ids, scales, near, far, arriving, *offsets):
    count, rows, _ = arriving.shape
    start = pl.program_id(0) * count

    @pl.when(ids[0] == 0)
    def _():
        def step(m):
            i = start + m
            at_rows = pl.ds(pl.multiple_of(m * rows, rows), rows)
            for j in range(SIDE):
                for inner in range(PER):
                    at = column(ids[2], j, inner)
                    hidden = f32(near[0, m, :, at]) * scale_at(
                        scales, 0, i, ids[2], j, inner
                    ) + f32(arriving[m, :, at])
                    behind = f32(far[0, m, :, at]) * scale_at(scales, 1, i, ids[2], j, inner)
                    offsets[j][at_rows, lanes(inner)] = (hidden - behind).astype(jnp.bfloat16)

        each_micro(count, step)


def multiply(phase, ids, rows, matrix, store):
    @pl.when(ids[0] == phase)
    def _():
        store(jnp.dot(rows, matrix[...], preferred_element_type=jnp.float32))

    @pl.when(ids[0] != phase)
    def _():
        store(
            lax.dot_general(
                rows, matrix[...], (((1,), (1,)), ((), ())), preferred_element_type=jnp.float32
            )
        )


def early_body(phase, ids, p0, p1, p3, matrix, *outs):
    for j, group in ((0, p0), (1, p1), (3, p3)):
        def store(product, j=j):
            count = product.shape[0] // SIDE
            for k in range(SIDE):
                outs[k][j] = product[k * count : (k + 1) * count].astype(jnp.bfloat16)

        multiply(phase, ids, group[...].reshape(-1, group.shape[-1]), matrix, store)


def late_body(phase, ids, low, high, matrix, *refs):
    outs = refs[SIDE:]
    rows = jnp.concatenate([low[0], low[1], high[0], high[1]], axis=0)

    def store(product):
        count = product.shape[0] // SIDE
        for k in range(SIDE):
            outs[k][0] = product[k * count : (k + 1) * count].astype(jnp.bfloat16)

    multiply(phase, ids, rows, matrix, store)


def combine_body(phase, ids, z0, z1, z2, z3, o0, o1, o2, o3, v0, v1, v2, v3, peak):
    offsets, outs = (o0, o1, o2, o3), (v0, v1, v2, v3)
    count = peak.shape[0]
    rows = z0.shape[1] // count
    forward = ids[0] == phase

    def step(m):
        at = pl.ds(pl.multiple_of(m * rows, rows), rows)
        for inner in range(PER):
            cols = lanes(inner)
            best = jnp.zeros((rows, BLOCK), jnp.float32)
            for j in range(SIDE):
                value = (f32(z0[j, at, cols]) + f32(z1[j, at, cols])) + (
                    f32(z2[j, at, cols]) + f32(z3[j, at, cols])
                )
                value = value + jnp.where(forward, f32(offsets[j][at, cols]), 0.0)
                outs[j][at, cols] = value.astype(jnp.bfloat16)
                best = jnp.maximum(best, jnp.abs(value))
            best = jnp.max(jnp.max(best, axis=0, keepdims=True), axis=1, keepdims=True)
            peak[m, :, cols] = jnp.broadcast_to(best, (1, BLOCK))

    each_micro(count, step)


def softened(delta, columns):
    spread = columns + epsilon
    level = delta * (code_levels / spread)
    part = level - jnp.round(level)
    square = part * part
    poly = jnp.full_like(square, SINE[-1])
    for coefficient in SINE[-2::-1]:
        poly = poly * square + coefficient
    sine = part * (0.25 - square) * poly
    smooth = level - (softness / two_pi) * sine
    return (smooth * (spread / code_levels)).astype(jnp.bfloat16)


def middle_body(ids, scales, *refs):
    own, other = refs[:SIDE], refs[SIDE : 2 * SIDE]
    own_peaks, other_peaks, between, cot = refs[2 * SIDE : 2 * SIDE + 4]
    outs = refs[2 * SIDE + 4 : 3 * SIDE + 4]
    sent, hidden, raw = refs[3 * SIDE + 4 :]
    count, rows, width = cot.shape
    start = pl.program_id(0) * count

    def step(m):
        i = start + m
        at_rows = pl.ds(pl.multiple_of(m * rows, rows), rows)

        def load(deltas, peaks, place):
            for j in range(SIDE):
                for inner in range(PER):
                    sent[m, :, column(place, j, inner)] = softened(
                        f32(deltas[j][at_rows, lanes(inner)]), peaks[j, i, :, lanes(inner)]
                    )

        def read(block, slot):
            at = lanes(block)
            return f32(between[0, m, :, at]) * (scales[slot, i, block] / code_levels) + f32(
                sent[m, :, at]
            )

        @pl.when(ids[0] == 0)
        def _():
            load(own, own_peaks, ids[2])
            for j in range(SIDE):
                for inner in range(PER):
                    raw[:, column(ids[1], j, inner)] = f32(other[j][at_rows, lanes(inner)])
            squares = jnp.zeros((rows, BLOCK), jnp.float32)
            crossed = jnp.zeros((rows, BLOCK), jnp.float32)
            for block in range(width // BLOCK):
                value = read(block, 1)
                hidden[:, lanes(block)] = value
                squares = squares + value * value
                crossed = crossed + value * raw[:, lanes(block)]
            inverse = root_mean(squares, width)
            mean = jnp.sum(crossed, axis=-1, keepdims=True) * (1.0 / width) * inverse * inverse
            for k in range(SIDE):
                for inner in range(PER):
                    at = column(ids[3], k, inner)
                    back = f32(cot[m, :, at]) + inverse * (raw[:, at] - hidden[:, at] * mean)
                    outs[k][at_rows, lanes(inner)] = back.astype(jnp.bfloat16)

        @pl.when(ids[0] != 0)
        def _():
            load(other, other_peaks, ids[1])
            squares = jnp.zeros((rows, BLOCK), jnp.float32)
            for block in range(width // BLOCK):
                value = read(block, 0)
                hidden[:, lanes(block)] = value
                squares = squares + value * value
            inverse = root_mean(squares, width)
            for k in range(SIDE):
                for inner in range(PER):
                    normed = hidden[:, column(ids[3], k, inner)] * inverse
                    outs[k][at_rows, lanes(inner)] = normed.astype(jnp.bfloat16)

    each_micro(count, step)


def middle_side_body(ids, scales, *refs):
    own, tokens = refs[:SIDE], refs[SIDE : 2 * SIDE]
    sent, near, far, cot = refs[2 * SIDE : 2 * SIDE + 4]
    offsets = refs[2 * SIDE + 4 : 3 * SIDE + 4]
    grads, hidden, raw = refs[3 * SIDE + 4 :]
    count, rows, width = cot.shape
    start = pl.program_id(0) * count

    @pl.when(ids[0] == 0)
    def _():
        def step(m):
            at_rows = pl.ds(pl.multiple_of(m * rows, rows), rows)
            for k in range(SIDE):
                for inner in range(PER):
                    at = column(ids[3], k, inner)
                    grads[m, :, at] = tokens[k][at_rows, lanes(inner)]

        each_micro(count, step)

    @pl.when(ids[0] != 0)
    def _():
        def step(m):
            i = start + m
            at_rows = pl.ds(pl.multiple_of(m * rows, rows), rows)
            for j in range(SIDE):
                for inner in range(PER):
                    raw[:, column(ids[2], j, inner)] = f32(own[j][at_rows, lanes(inner)])
            squares = jnp.zeros((rows, BLOCK), jnp.float32)
            crossed = jnp.zeros((rows, BLOCK), jnp.float32)
            for block in range(width // BLOCK):
                at = lanes(block)
                value = f32(near[0, m, :, at]) * (scales[0, i, block] / code_levels) + f32(
                    sent[m, :, at]
                )
                hidden[:, at] = value
                squares = squares + value * value
                crossed = crossed + value * raw[:, at]
            inverse = root_mean(squares, width)
            mean = jnp.sum(crossed, axis=-1, keepdims=True) * (1.0 / width) * inverse * inverse
            for block in range(width // BLOCK):
                at = lanes(block)
                back = f32(cot[m, :, at]) + inverse * (raw[:, at] - hidden[:, at] * mean)
                grads[m, :, at] = back.astype(jnp.bfloat16)
            for j in range(SIDE):
                for inner in range(PER):
                    at = column(ids[4], j, inner)
                    behind = f32(far[0, m, :, at]) * scale_at(scales, 1, i, ids[4], j, inner)
                    offsets[j][at_rows, lanes(inner)] = (hidden[:, at] - behind).astype(
                        jnp.bfloat16
                    )

        each_micro(count, step)


def last_body(ids, scales, r0, r1, r2, r3, peaks, near, arriving, upstream, sent, outs, grads, hidden, raw):
    result = (r0, r1, r2, r3)
    count, rows, width = arriving.shape
    start = pl.program_id(0) * count
    b = ids[4]

    @pl.when(ids[0] == 0)
    def _():
        def step(m):
            at_rows = pl.ds(pl.multiple_of(m * rows, rows), rows)
            for j in range(SIDE):
                for inner in range(PER):
                    raw[:, column(b, j, inner)] = f32(result[j][at_rows, lanes(inner)])
            squares = jnp.zeros((rows, BLOCK), jnp.float32)
            crossed = jnp.zeros((rows, BLOCK), jnp.float32)
            for block in range(width // BLOCK):
                at = lanes(block)
                value = f32(near[0, m, :, at]) * (
                    scales[0, start + m, block] / code_levels
                ) + f32(arriving[m, :, at])
                hidden[:, at] = value
                squares = squares + value * value
                crossed = crossed + value * raw[:, at]
            inverse = root_mean(squares, width)
            mean = jnp.sum(crossed, axis=-1, keepdims=True) * (1.0 / width) * inverse
            for block in range(width // BLOCK):
                at = lanes(block)
                unrounded = hidden[:, at] * inverse
                back = f32(upstream[m, :, at]) + inverse * (raw[:, at] - unrounded * mean)
                grads[m, :, at] = back.astype(jnp.bfloat16)

        each_micro(count, step)
        outs[...] = sent[...]

    @pl.when(ids[0] != 0)
    def _():
        def step(m):
            at_rows = pl.ds(pl.multiple_of(m * rows, rows), rows)
            for j in range(SIDE):
                for inner in range(PER):
                    outs[m, :, column(b, j, inner)] = softened(
                        f32(result[j][at_rows, lanes(inner)]),
                        peaks[j, start + m, :, lanes(inner)],
                    )

        each_micro(count, step)
        grads[...] = upstream[...]


def turn_body(ids, p0, p1, low, high, p3, out):
    rows = p0.shape[1]
    for i in range(SIDE):
        for j in range(SIDE):
            if j == 2:
                source = low[i] if i < 2 else high[i - 2]
            else:
                source = (p0, p1, None, p3)[j][i]
            at = (i * SIDE + j) * rows
            out[:, at : at + rows] = source.T


def gradient_body(ids, left, p0, p1, low, high, p3, *outs):
    span = left.shape[0]
    part = span // SIDE
    depth = left.shape[1] // SIDE
    for k in range(SIDE):
        columns = pl.ds(pl.multiple_of(lax.rem(ids[5] + k, SIDE) * part, part), part)
        total = jnp.zeros((span, part), jnp.float32)
        for i, groups in enumerate(((p0,), (p1,), (low, high), (p3,))):
            right = jnp.concatenate(
                [group[j, :, columns] for group in groups for j in range(group.shape[0])], axis=0
            )
            total = total + jnp.dot(
                left[:, i * depth : (i + 1) * depth], right, preferred_element_type=jnp.float32
            )
        outs[k][...] = total.astype(jnp.bfloat16)


def total_body(ids, q0, q1, q2, q3, *outs):
    part = q0.shape[1]
    for k in range(SIDE):
        row = jnp.where(ids[0] == 0, lax.rem(ids[5] + k, SIDE), k)
        at = pl.ds(pl.multiple_of(row * part, part), part)
        total = (f32(q0[at, :]) + f32(q1[at, :])) + (f32(q2[at, :]) + f32(q3[at, :]))
        outs[k][...] = total.astype(jnp.bfloat16)


def pass_body(ids, *refs):
    half = len(refs) // 2
    for source, target in zip(refs[:half], refs[half:]):
        target[...] = source[...]


def assemble_body(ids, g0, g1, g2, g3, out):
    depth = g0.shape[1]
    for l, group in enumerate((g0, g1, g2, g3)):
        for k in range(SIDE):
            row = lax.rem(ids[6] - k + SIDE, SIDE) * SIDE + lax.rem(ids[5] - l + SIDE, SIDE)
            out[pl.ds(pl.multiple_of(row * depth, depth), depth), :] = group[k]


def finish_body(ids, f0, f1, f2, f3, out):
    part = f0.shape[1]
    for k, piece in enumerate((f0, f1, f2, f3)):
        @pl.when(ids[0] == 0)
        def _():
            n = lax.rem(ids[6] - k + SIDE, SIDE)
            out[:, pl.ds(pl.multiple_of(n * part, part), part)] = f32(piece[...])

        @pl.when(ids[0] != 0)
        def _():
            out[:, k * part : (k + 1) * part] = f32(piece[...]).T


def local(in_delta, weight, cache_codes, cache_scales, cotangent):
    s = lax.axis_index("section")
    z = lax.axis_index("tensor_0")
    y = lax.axis_index("tensor_1")
    x = lax.axis_index("dp")
    micro_count, local_rows, width = in_delta.shape
    span = width // SIDE
    bf16, single = jnp.bfloat16, jnp.float32
    here = jnp.where(s == 0, z, y)
    there = jnp.where(s == 0, y, z)
    ids = jnp.stack([s, here, there, there, here, x, y]).astype(jnp.int32)

    count = micro_count // STEPS
    rows = micro_count * local_rows
    grid = (STEPS,)
    flat = (count, local_rows, width)
    in_smem = pl.BlockSpec(memory_space=pltpu.SMEM)
    piece = pl.BlockSpec((count * local_rows, span), lambda i, ids: (i, 0))
    piece_shape = jax.ShapeDtypeStruct((rows, span), bf16)
    whole = pl.BlockSpec(flat, lambda i, ids: (i, 0, 0))
    whole_shape = jax.ShapeDtypeStruct((micro_count, local_rows, width), bf16)
    work = [pltpu.VMEM((local_rows, width), single)]
    peak_shape = (micro_count, 1, span)
    peaks_spec = pl.BlockSpec((SIDE, *peak_shape), lambda i, ids: (0, 0, 0, 0))
    everything = pl.BlockSpec((SIDE, rows, span), lambda i, ids: (0, 0, 0))
    half = pl.BlockSpec((2, rows, span), lambda i, ids: (0, 0, 0))
    full_piece = pl.BlockSpec((rows, span), lambda i, ids: (0, 0))
    square = pl.BlockSpec((span, span), lambda i, ids: (0, 0))
    cut_shape = jax.ShapeDtypeStruct((SIDE, rows, span), bf16)
    codes, scales = cache_codes[0], cache_scales[0, :, :, 0, :]
    near = pl.BlockSpec((1, *flat), lambda i, ids: (0, i, 0, 0))
    far = pl.BlockSpec((1, *flat), lambda i, ids: (1, i, 0, 0))
    between = pl.BlockSpec((1, *flat), lambda i, ids: (1 - ids[0], i, 0, 0))

    depth = weight.shape[1] // SIDE

    def corner(k):
        return pl.BlockSpec((depth, span), lambda i, ids: (ids[5], lax.rem(ids[6] + k, SIDE)))

    quarters = call(
        pass_body,
        ids,
        (1,),
        [weight[0]] * SIDE,
        [corner(k) for k in range(SIDE)],
        [jax.ShapeDtypeStruct((depth, span), bf16)] * SIDE,
        [pl.BlockSpec((depth, span), lambda i, ids: (0, 0))] * SIDE,
    )
    quarter = jnp.stack([quarters[0]] + [ring(quarters[k], "tensor_1", k) for k in (1, 2, 3)])
    gathered = [quarter] + [ring(quarter, "dp", k) for k in (1, 2, 3)]
    block = call(
        assemble_body,
        ids,
        (1,),
        gathered,
        [pl.BlockSpec((SIDE, depth, span), lambda i, ids: (0, 0, 0))] * SIDE,
        jax.ShapeDtypeStruct((span, span), bf16),
        square,
    )

    def spread_out(pieces, phase):
        mine = jnp.stack([pieces[0]] + [shift(pieces[k], phase, "rows", k) for k in (1, 2, 3)])
        after = shift(mine, phase, "columns", 1)
        before = shift(mine, phase, "columns", -1)
        low = shift(after[:2], phase, "columns", 1)
        high = shift(before[2:], phase, "columns", -1)
        return [mine, after, low, high, before]

    def moved(offsets, phase):
        return [offsets[0]] + [shift(offsets[j], phase, "columns", j) for j in (1, 2, 3)]

    def products(groups, phase):
        made = call(
            functools.partial(early_body, phase),
            ids,
            (1,),
            [groups[0], groups[1], groups[4], block],
            [everything] * 3 + [square],
            [cut_shape] * SIDE,
            [everything] * SIDE,
            flops=6 * SIDE * rows * span * span,
        )
        late = pl.BlockSpec((1, rows, span), lambda i, ids: (2, 0, 0))
        made = call(
            functools.partial(late_body, phase),
            ids,
            (1,),
            [groups[2], groups[3], block, *made],
            [half, half, square] + [pl.BlockSpec(memory_space=pl.ANY)] * SIDE,
            [cut_shape] * SIDE,
            [late] * SIDE,
            flops=2 * SIDE * rows * span * span,
            aliases={4 + k: k for k in range(SIDE)},
        )
        return [made[0]] + [shift(made[k], phase, "rows", -k) for k in (1, 2, 3)]

    def returned(arrived, offsets, phase):
        *sent, peak = call(
            functools.partial(combine_body, phase),
            ids,
            (1,),
            [*arrived, *offsets],
            [everything] * SIDE + [full_piece] * SIDE,
            [piece_shape] * SIDE + [jax.ShapeDtypeStruct(peak_shape, single)],
            [full_piece] * SIDE + [pl.BlockSpec(peak_shape, lambda i, ids: (0, 0, 0))],
        )
        for k, other in [(k, shift(peak, phase, "rows", k)) for k in (1, 2, 3)]:
            peak = jnp.maximum(peak, other)
        home = [sent[0]] + [shift(sent[j], phase, "columns", -j) for j in (1, 2, 3)]
        peaks = jnp.stack([peak] + [shift(peak, phase, "columns", -j) for j in (1, 2, 3)])
        return home, peaks

    tokens = call(
        first_body,
        ids,
        grid,
        [scales, codes, in_delta, cotangent],
        [in_smem, near, whole, whole],
        [piece_shape] * SIDE,
        [piece] * SIDE,
        work,
    )
    groups = spread_out(tokens, 0)
    offsets = call(
        first_side_body,
        ids,
        grid,
        [scales, codes, codes, in_delta],
        [in_smem, near, far, whole],
        [piece_shape] * SIDE,
        [piece] * SIDE,
    )
    offsets = moved(offsets, 0)
    own, own_peaks = returned(products(groups, 0), offsets, 0)
    other_peaks = crossed_over(own_peaks)
    other = [crossed_over(own[j]) for j in range(SIDE)]
    *tokens, sent = call(
        middle_body,
        ids,
        grid,
        [scales, *own, *other, own_peaks, other_peaks, codes, cotangent],
        [in_smem] + [piece] * (2 * SIDE) + [peaks_spec, peaks_spec, between, whole],
        [piece_shape] * SIDE + [whole_shape],
        [piece] * SIDE + [whole],
        work * 2,
    )
    groups_next = spread_out(tokens, 1)
    *offsets, upstream = call(
        middle_side_body,
        ids,
        grid,
        [scales, *own, *tokens, sent, codes, codes, cotangent],
        [in_smem] + [piece] * (2 * SIDE) + [whole, near, far, whole],
        [piece_shape] * SIDE + [whole_shape],
        [piece] * SIDE + [whole],
        work * 2,
    )
    offsets = moved(offsets, 1)
    result, peaks = returned(products(groups_next, 1), offsets, 1)
    outs, grads = call(
        last_body,
        ids,
        grid,
        [scales, *result, peaks, codes, in_delta, upstream, sent],
        [in_smem] + [piece] * SIDE + [peaks_spec, near, whole, whole, whole],
        [whole_shape, whole_shape],
        [whole, whole],
        work * 2,
    )

    total_rows = SIDE * SIDE * rows
    part = span // SIDE
    gathered_specs = [everything, everything, half, half, everything]
    tall = pl.BlockSpec((span, part), lambda i, ids: (0, 0))
    small = pl.BlockSpec((part, part), lambda i, ids: (0, 0))
    flipped = pl.BlockSpec((span, total_rows), lambda i, ids: (0, 0))
    left = call(
        turn_body,
        ids,
        (1,),
        groups,
        gathered_specs,
        jax.ShapeDtypeStruct((span, total_rows), bf16),
        flipped,
    )
    partials = call(
        gradient_body,
        ids,
        (1,),
        [left, *groups_next],
        [flipped, *gathered_specs],
        [jax.ShapeDtypeStruct((span, part), bf16)] * SIDE,
        [tall] * SIDE,
        flops=2 * total_rows * span * span,
    )
    arrived = [partials[0]] + [ring(partials[k], "dp", k) for k in (1, 2, 3)]
    pieces = call(
        total_body,
        ids,
        (1,),
        arrived,
        [tall] * SIDE,
        [jax.ShapeDtypeStruct((part, part), bf16)] * SIDE,
        [small] * SIDE,
    )
    pieces = [to_owner(pieces[k], k) for k in range(SIDE)]
    weight_grad = call(
        finish_body,
        ids,
        (1,),
        pieces,
        [small] * SIDE,
        jax.ShapeDtypeStruct((part, span), single),
        pl.BlockSpec((part, span), lambda i, ids: (0, 0)),
    )
    return outs[None], grads[None], weight_grad[None]


def solution(mesh):
    finer = Mesh(
        mesh.devices.reshape(mesh.shape["dp"], mesh.shape["section"], SIDE, SIDE),
        ("dp", "section", "tensor_0", "tensor_1"),
    )
    return jax.shard_map(
        local,
        mesh=finer,
        in_specs=(
            P(None, DP_TENSOR, None),
            P("section", TENSOR, None),
            P("section", None, None, DP_TENSOR, None),
            P("section", None, None, "dp", None),
            P(None, DP_TENSOR, None),
        ),
        out_specs=(
            P("section", None, DP_TENSOR, None),
            P("section", None, DP_TENSOR, None),
            P("section", TENSOR, "dp"),
        ),
        check_vma=False,
    )
```

```python
import functools

import jax
import jax.numpy as jnp
from jax import lax
from jax.experimental import pallas as pl
from jax.experimental.pallas import tpu as pltpu
from jax.sharding import Mesh
from jax.sharding import PartitionSpec as P


TENSOR = ("tensor_0", "tensor_1")
CHIP = ("section", "tensor_0", "tensor_1")
DP_TENSOR = ("dp", "tensor_0", "tensor_1")
SIDE = 4
BLOCK = 128
PER = 8
STEPS = 2
VMEM_LIMIT = 24 * 1024 * 1024

code_levels = 7.0
softness = 0.8
two_pi = 6.283185307179586
epsilon = 1e-06

SINE = (25.13274118, -64.8358279, 67.07681018, -38.49815464, 14.06107271, -3.181409966)


def on_z(s, phase, along):
    return ((s + phase) % 2 == 0) == (along == "rows")


def position(s, z, y):
    return (s * SIDE + z) * SIDE + y


def shift(value, phase, along, steps):
    pairs = []
    for s in range(2):
        for z in range(SIDE):
            for y in range(SIDE):
                if on_z(s, phase, along):
                    target = position(s, (z + steps) % SIDE, y)
                else:
                    target = position(s, z, (y + steps) % SIDE)
                pairs.append((position(s, z, y), target))
    return lax.ppermute(value, CHIP, pairs)


def ring(value, axis, steps):
    return lax.ppermute(value, axis, [(i, (i + steps) % SIDE) for i in range(SIDE)])


def crossed_over(value):
    return lax.ppermute(value, "section", [(0, 1), (1, 0)])


def lanes(block):
    return slice(block * BLOCK, (block + 1) * BLOCK)


def f32(value):
    return value.astype(jnp.float32)


def call(body, ids, grid, inputs, in_specs, shapes, out_specs, scratch=(), flops=0, aliases=None):
    cost = pl.CostEstimate(flops=flops or 20_000_000, bytes_accessed=8_000_000, transcendentals=0)
    return pl.pallas_call(
        body,
        grid_spec=pltpu.PrefetchScalarGridSpec(
            num_scalar_prefetch=1,
            grid=grid,
            in_specs=in_specs,
            out_specs=out_specs,
            scratch_shapes=scratch,
        ),
        out_shape=shapes,
        cost_estimate=cost,
        compiler_params=pltpu.CompilerParams(vmem_limit_bytes=VMEM_LIMIT),
        input_output_aliases=aliases or {},
    )(ids, *inputs)


def root_mean(squares, width):
    return lax.rsqrt(jnp.sum(squares, axis=-1, keepdims=True) * (1.0 / width) + epsilon)


def column(place, steps, inner):
    n = lax.rem(place + steps + SIDE, SIDE)
    return pl.ds(pl.multiple_of(n * PER * BLOCK + inner * BLOCK, BLOCK), BLOCK)


def scale_at(scales, slot, micro, place, steps, inner):
    n = lax.rem(place + steps + SIDE, SIDE)
    return scales[slot, micro, n * PER + inner] / code_levels


def each_micro(count, step):
    lax.fori_loop(0, count, lambda m, _: (step(m), None)[1], None)


def first_body(ids, scales, near, arriving, cot, *refs):
    outs, hidden = refs[:SIDE], refs[SIDE]
    count, rows, width = arriving.shape
    start = pl.program_id(0) * count

    @pl.when(ids[0] == 0)
    def _():
        def step(m):
            i = start + m
            at_rows = pl.ds(pl.multiple_of(m * rows, rows), rows)
            squares = jnp.zeros((rows, BLOCK), jnp.float32)
            for block in range(width // BLOCK):
                at = lanes(block)
                value = f32(near[0, m, :, at]) * (scales[0, i, block] / code_levels) + f32(
                    arriving[m, :, at]
                )
                hidden[:, at] = value
                squares = squares + value * value
            inverse = root_mean(squares, width)
            for k in range(SIDE):
                for inner in range(PER):
                    normed = hidden[:, column(ids[1], k, inner)] * inverse
                    outs[k][at_rows, lanes(inner)] = normed.astype(jnp.bfloat16)

        each_micro(count, step)

    @pl.when(ids[0] != 0)
    def _():
        def step(m):
            at_rows = pl.ds(pl.multiple_of(m * rows, rows), rows)
            for k in range(SIDE):
                for inner in range(PER):
                    outs[k][at_rows, lanes(inner)] = cot[m, :, column(ids[1], k, inner)]

        each_micro(count, step)


def first_side_body(ids, scales, near, far, arriving, *offsets):
    count, rows, _ = arriving.shape
    start = pl.program_id(0) * count

    @pl.when(ids[0] == 0)
    def _():
        def step(m):
            i = start + m
            at_rows = pl.ds(pl.multiple_of(m * rows, rows), rows)
            for j in range(SIDE):
                for inner in range(PER):
                    at = column(ids[2], j, inner)
                    hidden = f32(near[0, m, :, at]) * scale_at(
                        scales, 0, i, ids[2], j, inner
                    ) + f32(arriving[m, :, at])
                    behind = f32(far[0, m, :, at]) * scale_at(scales, 1, i, ids[2], j, inner)
                    offsets[j][at_rows, lanes(inner)] = (hidden - behind).astype(jnp.bfloat16)

        each_micro(count, step)


def tile(n, size):
    return pl.ds(pl.multiple_of(n * size, size), size)


def multiply(phase, ids, read, matrix, store):
    part = matrix.shape[0] // SIDE

    @pl.when(ids[0] == phase)
    def _():
        def step(n):
            cols = tile(n, part)
            store(jnp.dot(read(), matrix[:, cols], preferred_element_type=jnp.float32), cols)

        each_micro(SIDE, step)

    @pl.when(ids[0] != phase)
    def _():
        def step(n):
            cols = tile(n, part)
            product = lax.dot_general(
                read(), matrix[cols, :], (((1,), (1,)), ((), ())), preferred_element_type=jnp.float32
            )
            store(product, cols)

        each_micro(SIDE, step)


def early_body(phase, ids, p0, p1, p3, matrix, *outs):
    for j, group in ((0, p0), (1, p1), (3, p3)):
        def read(group=group):
            return group[...].reshape(-1, group.shape[-1])

        def store(product, cols, j=j):
            count = product.shape[0] // SIDE
            for k in range(SIDE):
                outs[k][j, :, cols] = product[k * count : (k + 1) * count].astype(jnp.bfloat16)

        multiply(phase, ids, read, matrix, store)


def late_body(phase, ids, low, high, matrix, *refs):
    outs = refs[SIDE:]

    def read():
        return jnp.concatenate([low[0], low[1], high[0], high[1]], axis=0)

    def store(product, cols):
        count = product.shape[0] // SIDE
        for k in range(SIDE):
            outs[k][0, :, cols] = product[k * count : (k + 1) * count].astype(jnp.bfloat16)

    multiply(phase, ids, read, matrix, store)


def combine_body(phase, ids, z0, z1, z2, z3, o0, o1, o2, o3, v0, v1, v2, v3, peak):
    offsets, outs = (o0, o1, o2, o3), (v0, v1, v2, v3)
    count = peak.shape[0]
    rows = z0.shape[1] // count
    forward = ids[0] == phase

    def step(m):
        at = pl.ds(pl.multiple_of(m * rows, rows), rows)
        for inner in range(PER):
            cols = lanes(inner)
            best = jnp.zeros((rows, BLOCK), jnp.float32)
            for j in range(SIDE):
                value = (f32(z0[j, at, cols]) + f32(z1[j, at, cols])) + (
                    f32(z2[j, at, cols]) + f32(z3[j, at, cols])
                )
                value = value + jnp.where(forward, f32(offsets[j][at, cols]), 0.0)
                outs[j][at, cols] = value.astype(jnp.bfloat16)
                best = jnp.maximum(best, jnp.abs(value))
            best = jnp.max(jnp.max(best, axis=0, keepdims=True), axis=1, keepdims=True)
            peak[m, :, cols] = jnp.broadcast_to(best, (1, BLOCK))

    each_micro(count, step)


def softened(delta, columns):
    spread = columns + epsilon
    level = delta * (code_levels / spread)
    part = level - jnp.round(level)
    square = part * part
    poly = jnp.full_like(square, SINE[-1])
    for coefficient in SINE[-2::-1]:
        poly = poly * square + coefficient
    sine = part * (0.25 - square) * poly
    smooth = level - (softness / two_pi) * sine
    return (smooth * (spread / code_levels)).astype(jnp.bfloat16)


def middle_body(ids, scales, *refs):
    own, other = refs[:SIDE], refs[SIDE : 2 * SIDE]
    own_peaks, other_peaks, between, cot = refs[2 * SIDE : 2 * SIDE + 4]
    outs = refs[2 * SIDE + 4 : 3 * SIDE + 4]
    sent, hidden, raw = refs[3 * SIDE + 4 :]
    count, rows, width = cot.shape
    start = pl.program_id(0) * count

    def step(m):
        i = start + m
        at_rows = pl.ds(pl.multiple_of(m * rows, rows), rows)

        def load(deltas, peaks, place):
            for j in range(SIDE):
                for inner in range(PER):
                    sent[m, :, column(place, j, inner)] = softened(
                        f32(deltas[j][at_rows, lanes(inner)]), peaks[j, i, :, lanes(inner)]
                    )

        def read(block, slot):
            at = lanes(block)
            return f32(between[0, m, :, at]) * (scales[slot, i, block] / code_levels) + f32(
                sent[m, :, at]
            )

        @pl.when(ids[0] == 0)
        def _():
            load(own, own_peaks, ids[2])
            for j in range(SIDE):
                for inner in range(PER):
                    raw[:, column(ids[1], j, inner)] = f32(other[j][at_rows, lanes(inner)])
            squares = jnp.zeros((rows, BLOCK), jnp.float32)
            crossed = jnp.zeros((rows, BLOCK), jnp.float32)
            for block in range(width // BLOCK):
                value = read(block, 1)
                hidden[:, lanes(block)] = value
                squares = squares + value * value
                crossed = crossed + value * raw[:, lanes(block)]
            inverse = root_mean(squares, width)
            mean = jnp.sum(crossed, axis=-1, keepdims=True) * (1.0 / width) * inverse * inverse
            for k in range(SIDE):
                for inner in range(PER):
                    at = column(ids[3], k, inner)
                    back = f32(cot[m, :, at]) + inverse * (raw[:, at] - hidden[:, at] * mean)
                    outs[k][at_rows, lanes(inner)] = back.astype(jnp.bfloat16)

        @pl.when(ids[0] != 0)
        def _():
            load(other, other_peaks, ids[1])
            squares = jnp.zeros((rows, BLOCK), jnp.float32)
            for block in range(width // BLOCK):
                value = read(block, 0)
                hidden[:, lanes(block)] = value
                squares = squares + value * value
            inverse = root_mean(squares, width)
            for k in range(SIDE):
                for inner in range(PER):
                    normed = hidden[:, column(ids[3], k, inner)] * inverse
                    outs[k][at_rows, lanes(inner)] = normed.astype(jnp.bfloat16)

    each_micro(count, step)


def middle_side_body(ids, scales, *refs):
    own, tokens = refs[:SIDE], refs[SIDE : 2 * SIDE]
    sent, near, far, cot = refs[2 * SIDE : 2 * SIDE + 4]
    offsets = refs[2 * SIDE + 4 : 3 * SIDE + 4]
    grads, hidden, raw = refs[3 * SIDE + 4 :]
    count, rows, width = cot.shape
    start = pl.program_id(0) * count

    @pl.when(ids[0] == 0)
    def _():
        def step(m):
            at_rows = pl.ds(pl.multiple_of(m * rows, rows), rows)
            for k in range(SIDE):
                for inner in range(PER):
                    at = column(ids[3], k, inner)
                    grads[m, :, at] = tokens[k][at_rows, lanes(inner)]

        each_micro(count, step)

    @pl.when(ids[0] != 0)
    def _():
        def step(m):
            i = start + m
            at_rows = pl.ds(pl.multiple_of(m * rows, rows), rows)
            for j in range(SIDE):
                for inner in range(PER):
                    raw[:, column(ids[2], j, inner)] = f32(own[j][at_rows, lanes(inner)])
            squares = jnp.zeros((rows, BLOCK), jnp.float32)
            crossed = jnp.zeros((rows, BLOCK), jnp.float32)
            for block in range(width // BLOCK):
                at = lanes(block)
                value = f32(near[0, m, :, at]) * (scales[0, i, block] / code_levels) + f32(
                    sent[m, :, at]
                )
                hidden[:, at] = value
                squares = squares + value * value
                crossed = crossed + value * raw[:, at]
            inverse = root_mean(squares, width)
            mean = jnp.sum(crossed, axis=-1, keepdims=True) * (1.0 / width) * inverse * inverse
            for block in range(width // BLOCK):
                at = lanes(block)
                back = f32(cot[m, :, at]) + inverse * (raw[:, at] - hidden[:, at] * mean)
                grads[m, :, at] = back.astype(jnp.bfloat16)
            for j in range(SIDE):
                for inner in range(PER):
                    at = column(ids[4], j, inner)
                    behind = f32(far[0, m, :, at]) * scale_at(scales, 1, i, ids[4], j, inner)
                    offsets[j][at_rows, lanes(inner)] = (hidden[:, at] - behind).astype(
                        jnp.bfloat16
                    )

        each_micro(count, step)


def last_body(ids, scales, r0, r1, r2, r3, peaks, near, arriving, upstream, sent, outs, grads, hidden, raw):
    result = (r0, r1, r2, r3)
    count, rows, width = arriving.shape
    start = pl.program_id(0) * count
    b = ids[4]

    @pl.when(ids[0] == 0)
    def _():
        def step(m):
            at_rows = pl.ds(pl.multiple_of(m * rows, rows), rows)
            for j in range(SIDE):
                for inner in range(PER):
                    raw[:, column(b, j, inner)] = f32(result[j][at_rows, lanes(inner)])
            squares = jnp.zeros((rows, BLOCK), jnp.float32)
            crossed = jnp.zeros((rows, BLOCK), jnp.float32)
            for block in range(width // BLOCK):
                at = lanes(block)
                value = f32(near[0, m, :, at]) * (
                    scales[0, start + m, block] / code_levels
                ) + f32(arriving[m, :, at])
                hidden[:, at] = value
                squares = squares + value * value
                crossed = crossed + value * raw[:, at]
            inverse = root_mean(squares, width)
            mean = jnp.sum(crossed, axis=-1, keepdims=True) * (1.0 / width) * inverse
            for block in range(width // BLOCK):
                at = lanes(block)
                unrounded = hidden[:, at] * inverse
                back = f32(upstream[m, :, at]) + inverse * (raw[:, at] - unrounded * mean)
                grads[m, :, at] = back.astype(jnp.bfloat16)

        each_micro(count, step)
        outs[...] = sent[...]

    @pl.when(ids[0] != 0)
    def _():
        def step(m):
            at_rows = pl.ds(pl.multiple_of(m * rows, rows), rows)
            for j in range(SIDE):
                for inner in range(PER):
                    outs[m, :, column(b, j, inner)] = softened(
                        f32(result[j][at_rows, lanes(inner)]),
                        peaks[j, start + m, :, lanes(inner)],
                    )

        each_micro(count, step)
        grads[...] = upstream[...]


def turn_body(ids, p0, p1, low, high, p3, out):
    rows = p0.shape[1]
    for i in range(SIDE):
        for j in range(SIDE):
            if j == 2:
                source = low[i] if i < 2 else high[i - 2]
            else:
                source = (p0, p1, None, p3)[j][i]
            at = (i * SIDE + j) * rows
            out[:, at : at + rows] = source.T


def gradient_body(ids, left, p0, p1, low, high, p3, *outs):
    span = left.shape[0]
    part = span // SIDE
    depth = left.shape[1] // SIDE

    def product(rows, columns):
        total = None
        for i, groups in enumerate(((p0,), (p1,), (low, high), (p3,))):
            right = jnp.concatenate(
                [group[j, :, columns] for group in groups for j in range(group.shape[0])], axis=0
            )
            term = jnp.dot(
                left[rows, i * depth : (i + 1) * depth], right, preferred_element_type=jnp.float32
            )
            total = term if total is None else total + term
        return total.astype(jnp.bfloat16)

    for k in range(SIDE):
        mine = tile(lax.rem(ids[5] + k, SIDE), part)

        @pl.when(ids[0] == 0)
        def _():
            def step(n):
                outs[k][tile(n, part), :] = product(tile(n, part), mine)

            each_micro(SIDE, step)

        @pl.when(ids[0] != 0)
        def _():
            def step(n):
                outs[k][tile(n, part), :] = product(mine, tile(n, part)).T

            each_micro(SIDE, step)


def total_body(ids, q0, q1, q2, q3, *outs):
    part = q0.shape[1]
    for k in range(SIDE):
        at = tile(lax.rem(ids[6] + k, SIDE), part)
        total = (f32(q0[at, :]) + f32(q1[at, :])) + (f32(q2[at, :]) + f32(q3[at, :]))
        outs[k][...] = total.astype(jnp.bfloat16)


def choose_body(ids, r0, r1, r2, r3, *outs):
    for l in range(SIDE):
        k = lax.rem(ids[6] - ids[5] - l + 2 * SIDE, SIDE)
        for at, source in enumerate((r0, r1, r2, r3)):
            @pl.when(k == at)
            def _():
                outs[l][...] = source[...]


def pass_body(ids, *refs):
    half = len(refs) // 2
    for source, target in zip(refs[:half], refs[half:]):
        target[...] = source[...]


def assemble_body(ids, a0, b0, a1, b1, out):
    depth = a0.shape[1]
    odd = lax.rem(ids[5], 2)
    for k in range(SIDE):
        row = lax.rem(ids[6] - k + SIDE, SIDE) * SIDE
        for at, group in ((2 * odd, a0), (2 * odd + 1, b0), (2 - 2 * odd, a1), (3 - 2 * odd, b1)):
            out[tile(row + at, depth), :] = group[k]


def finish_body(ids, f0, f1, f2, f3, out):
    part = f0.shape[1]
    for l, piece in enumerate((f0, f1, f2, f3)):
        out[:, tile(lax.rem(ids[5] - l + SIDE, SIDE), part)] = f32(piece[...])


def local(in_delta, weight, cache_codes, cache_scales, cotangent):
    s = lax.axis_index("section")
    z = lax.axis_index("tensor_0")
    y = lax.axis_index("tensor_1")
    x = lax.axis_index("dp")
    micro_count, local_rows, width = in_delta.shape
    span = width // SIDE
    bf16, single = jnp.bfloat16, jnp.float32
    here = jnp.where(s == 0, z, y)
    there = jnp.where(s == 0, y, z)
    ids = jnp.stack([s, here, there, there, here, x, y]).astype(jnp.int32)

    count = micro_count // STEPS
    rows = micro_count * local_rows
    grid = (STEPS,)
    flat = (count, local_rows, width)
    in_smem = pl.BlockSpec(memory_space=pltpu.SMEM)
    piece = pl.BlockSpec((count * local_rows, span), lambda i, ids: (i, 0))
    piece_shape = jax.ShapeDtypeStruct((rows, span), bf16)
    whole = pl.BlockSpec(flat, lambda i, ids: (i, 0, 0))
    whole_shape = jax.ShapeDtypeStruct((micro_count, local_rows, width), bf16)
    work = [pltpu.VMEM((local_rows, width), single)]
    peak_shape = (micro_count, 1, span)
    peaks_spec = pl.BlockSpec((SIDE, *peak_shape), lambda i, ids: (0, 0, 0, 0))
    everything = pl.BlockSpec((SIDE, rows, span), lambda i, ids: (0, 0, 0))
    half = pl.BlockSpec((2, rows, span), lambda i, ids: (0, 0, 0))
    full_piece = pl.BlockSpec((rows, span), lambda i, ids: (0, 0))
    square = pl.BlockSpec((span, span), lambda i, ids: (0, 0))
    cut_shape = jax.ShapeDtypeStruct((SIDE, rows, span), bf16)
    codes, scales = cache_codes[0], cache_scales[0, :, :, 0, :]
    near = pl.BlockSpec((1, *flat), lambda i, ids: (0, i, 0, 0))
    far = pl.BlockSpec((1, *flat), lambda i, ids: (1, i, 0, 0))
    between = pl.BlockSpec((1, *flat), lambda i, ids: (1 - ids[0], i, 0, 0))

    depth = weight.shape[1] // 2

    def corner(k):
        return pl.BlockSpec(
            (depth, span), lambda i, ids: (lax.rem(ids[5], 2), lax.rem(ids[6] + k, SIDE))
        )

    halves = call(
        pass_body,
        ids,
        (1,),
        [weight[0]] * SIDE,
        [corner(k) for k in range(SIDE)],
        [jax.ShapeDtypeStruct((depth, span), bf16)] * SIDE,
        [pl.BlockSpec((depth, span), lambda i, ids: (0, 0))] * SIDE,
    )
    halves = [halves[0]] + [ring(halves[k], "tensor_1", k) for k in (1, 2, 3)]
    upper = jnp.stack([part[: depth // 2] for part in halves])
    lower = jnp.stack([part[depth // 2 :] for part in halves])
    block = call(
        assemble_body,
        ids,
        (1,),
        [upper, lower, ring(upper, "dp", 1), ring(lower, "dp", -1)],
        [pl.BlockSpec((SIDE, depth // 2, span), lambda i, ids: (0, 0, 0))] * SIDE,
        jax.ShapeDtypeStruct((span, span), bf16),
        square,
    )

    def spread_out(pieces, phase):
        mine = jnp.stack([pieces[0]] + [shift(pieces[k], phase, "rows", k) for k in (1, 2, 3)])
        after = shift(mine, phase, "columns", 1)
        before = shift(mine, phase, "columns", -1)
        low = shift(after[:2], phase, "columns", 1)
        high = shift(before[2:], phase, "columns", -1)
        return [mine, after, low, high, before]

    def moved(offsets, phase):
        return [offsets[0]] + [shift(offsets[j], phase, "columns", j) for j in (1, 2, 3)]

    def products(groups, phase):
        made = call(
            functools.partial(early_body, phase),
            ids,
            (1,),
            [groups[0], groups[1], groups[4], block],
            [everything] * 3 + [square],
            [cut_shape] * SIDE,
            [everything] * SIDE,
            flops=6 * SIDE * rows * span * span,
        )
        late = pl.BlockSpec((1, rows, span), lambda i, ids: (2, 0, 0))
        made = call(
            functools.partial(late_body, phase),
            ids,
            (1,),
            [groups[2], groups[3], block, *made],
            [half, half, square] + [pl.BlockSpec(memory_space=pl.ANY)] * SIDE,
            [cut_shape] * SIDE,
            [late] * SIDE,
            flops=2 * SIDE * rows * span * span,
            aliases={4 + k: k for k in range(SIDE)},
        )
        return [made[0]] + [shift(made[k], phase, "rows", -k) for k in (1, 2, 3)]

    def returned(arrived, offsets, phase):
        *sent, peak = call(
            functools.partial(combine_body, phase),
            ids,
            (1,),
            [*arrived, *offsets],
            [everything] * SIDE + [full_piece] * SIDE,
            [piece_shape] * SIDE + [jax.ShapeDtypeStruct(peak_shape, single)],
            [full_piece] * SIDE + [pl.BlockSpec(peak_shape, lambda i, ids: (0, 0, 0))],
        )
        for k, other in [(k, shift(peak, phase, "rows", k)) for k in (1, 2, 3)]:
            peak = jnp.maximum(peak, other)
        home = [sent[0]] + [shift(sent[j], phase, "columns", -j) for j in (1, 2, 3)]
        peaks = jnp.stack([peak] + [shift(peak, phase, "columns", -j) for j in (1, 2, 3)])
        return home, peaks

    tokens = call(
        first_body,
        ids,
        grid,
        [scales, codes, in_delta, cotangent],
        [in_smem, near, whole, whole],
        [piece_shape] * SIDE,
        [piece] * SIDE,
        work,
    )
    groups = spread_out(tokens, 0)
    offsets = call(
        first_side_body,
        ids,
        grid,
        [scales, codes, codes, in_delta],
        [in_smem, near, far, whole],
        [piece_shape] * SIDE,
        [piece] * SIDE,
    )
    offsets = moved(offsets, 0)
    own, own_peaks = returned(products(groups, 0), offsets, 0)
    other_peaks = crossed_over(own_peaks)
    other = [crossed_over(own[j]) for j in range(SIDE)]
    *tokens, sent = call(
        middle_body,
        ids,
        grid,
        [scales, *own, *other, own_peaks, other_peaks, codes, cotangent],
        [in_smem] + [piece] * (2 * SIDE) + [peaks_spec, peaks_spec, between, whole],
        [piece_shape] * SIDE + [whole_shape],
        [piece] * SIDE + [whole],
        work * 2,
    )
    groups_next = spread_out(tokens, 1)
    *offsets, upstream = call(
        middle_side_body,
        ids,
        grid,
        [scales, *own, *tokens, sent, codes, codes, cotangent],
        [in_smem] + [piece] * (2 * SIDE) + [whole, near, far, whole],
        [piece_shape] * SIDE + [whole_shape],
        [piece] * SIDE + [whole],
        work * 2,
    )
    offsets = moved(offsets, 1)
    result, peaks = returned(products(groups_next, 1), offsets, 1)
    outs, grads = call(
        last_body,
        ids,
        grid,
        [scales, *result, peaks, codes, in_delta, upstream, sent],
        [in_smem] + [piece] * SIDE + [peaks_spec, near, whole, whole, whole],
        [whole_shape, whole_shape],
        [whole, whole],
        work * 2,
    )

    total_rows = SIDE * SIDE * rows
    part = span // SIDE
    gathered_specs = [everything, everything, half, half, everything]
    tall = pl.BlockSpec((span, part), lambda i, ids: (0, 0))
    small = pl.BlockSpec((part, part), lambda i, ids: (0, 0))
    flipped = pl.BlockSpec((span, total_rows), lambda i, ids: (0, 0))
    left = call(
        turn_body,
        ids,
        (1,),
        groups,
        gathered_specs,
        jax.ShapeDtypeStruct((span, total_rows), bf16),
        flipped,
    )
    partials = call(
        gradient_body,
        ids,
        (1,),
        [left, *groups_next],
        [flipped, *gathered_specs],
        [jax.ShapeDtypeStruct((span, part), bf16)] * SIDE,
        [tall] * SIDE,
        flops=2 * total_rows * span * span,
    )
    arrived = [partials[0]] + [ring(partials[k], "dp", k) for k in (1, 2, 3)]
    pieces = call(
        total_body,
        ids,
        (1,),
        arrived,
        [tall] * SIDE,
        [jax.ShapeDtypeStruct((part, part), bf16)] * SIDE,
        [small] * SIDE,
    )
    pieces = [pieces[0]] + [ring(pieces[k], "tensor_1", k) for k in (1, 2, 3)]
    pieces = call(
        choose_body,
        ids,
        (1,),
        pieces,
        [small] * SIDE,
        [jax.ShapeDtypeStruct((part, part), bf16)] * SIDE,
        [small] * SIDE,
    )
    pieces = [pieces[0]] + [ring(pieces[k], "dp", k) for k in (1, 2, 3)]
    weight_grad = call(
        finish_body,
        ids,
        (1,),
        pieces,
        [small] * SIDE,
        jax.ShapeDtypeStruct((part, span), single),
        pl.BlockSpec((part, span), lambda i, ids: (0, 0)),
    )
    return outs[None], grads[None], weight_grad[None]


def solution(mesh):
    finer = Mesh(
        mesh.devices.reshape(mesh.shape["dp"], mesh.shape["section"], SIDE, SIDE),
        ("dp", "section", "tensor_0", "tensor_1"),
    )
    return jax.shard_map(
        local,
        mesh=finer,
        in_specs=(
            P(None, DP_TENSOR, None),
            P("section", TENSOR, None),
            P("section", None, None, DP_TENSOR, None),
            P("section", None, None, "dp", None),
            P(None, DP_TENSOR, None),
        ),
        out_specs=(
            P("section", None, DP_TENSOR, None),
            P("section", None, DP_TENSOR, None),
            P("section", TENSOR, "dp"),
        ),
        check_vma=False,
    )
```

```python
import functools

import jax
import jax.numpy as jnp
from jax import lax
from jax.experimental import pallas as pl
from jax.experimental.pallas import tpu as pltpu
from jax.sharding import Mesh
from jax.sharding import PartitionSpec as P


TENSOR = ("tensor_0", "tensor_1")
CHIP = ("section", "tensor_0", "tensor_1")
DP_TENSOR = ("dp", "tensor_0", "tensor_1")
SIDE = 4
ROWS, COLUMNS = "rows", "columns"
DP, SECTION, FAST = "dp", "section", "tensor_1"
BLOCK = 128
PER = 8
STEPS = 2
VMEM_LIMIT = 24 * 1024 * 1024

code_levels = 7.0
softness = 0.8
two_pi = 6.283185307179586
epsilon = 1e-06

SINE = (25.13274118, -64.8358279, 67.07681018, -38.49815464, 14.06107271, -3.181409966)


def on_z(s, phase, along):
    return ((s + phase) % 2 == 0) == (along == ROWS)


def position(s, z, y):
    return (s * SIDE + z) * SIDE + y


def shift(value, phase, along, steps):
    pairs = []
    for s in range(2):
        for z in range(SIDE):
            for y in range(SIDE):
                if on_z(s, phase, along):
                    target = position(s, (z + steps) % SIDE, y)
                else:
                    target = position(s, z, (y + steps) % SIDE)
                pairs.append((position(s, z, y), target))
    return lax.ppermute(value, CHIP, pairs)


def ring(value, axis, steps):
    return lax.ppermute(value, axis, [(i, (i + steps) % SIDE) for i in range(SIDE)])


def crossed_over(value):
    return lax.ppermute(value, SECTION, [(0, 1), (1, 0)])


def lanes(block):
    return slice(block * BLOCK, (block + 1) * BLOCK)


def f32(value):
    return value.astype(jnp.float32)


def call(body, ids, grid, inputs, in_specs, shapes, out_specs, scratch=(), flops=0, aliases=None):
    cost = pl.CostEstimate(flops=flops or 20_000_000, bytes_accessed=8_000_000, transcendentals=0)
    return pl.pallas_call(
        body,
        grid_spec=pltpu.PrefetchScalarGridSpec(
            num_scalar_prefetch=1,
            grid=grid,
            in_specs=in_specs,
            out_specs=out_specs,
            scratch_shapes=scratch,
        ),
        out_shape=shapes,
        cost_estimate=cost,
        compiler_params=pltpu.CompilerParams(vmem_limit_bytes=VMEM_LIMIT),
        input_output_aliases=aliases or {},
    )(ids, *inputs)


def root_mean(squares, width):
    return lax.rsqrt(jnp.sum(squares, axis=-1, keepdims=True) * (1.0 / width) + epsilon)


def column(place, steps, inner):
    n = lax.rem(place + steps + SIDE, SIDE)
    return pl.ds(pl.multiple_of(n * PER * BLOCK + inner * BLOCK, BLOCK), BLOCK)


def scale_at(scales, slot, micro, place, steps, inner):
    n = lax.rem(place + steps + SIDE, SIDE)
    return scales[slot, micro, n * PER + inner] / code_levels


def each_micro(count, step):
    lax.fori_loop(0, count, lambda m, _: (step(m), None)[1], None)


def first_body(ids, scales, near, arriving, cot, *refs):
    outs, hidden = refs[:SIDE], refs[SIDE]
    count, rows, width = arriving.shape
    start = pl.program_id(0) * count

    @pl.when(ids[0] == 0)
    def _():
        def step(m):
            i = start + m
            at_rows = pl.ds(pl.multiple_of(m * rows, rows), rows)
            squares = jnp.zeros((rows, BLOCK), jnp.float32)
            for block in range(width // BLOCK):
                at = lanes(block)
                value = f32(near[0, m, :, at]) * (scales[0, i, block] / code_levels) + f32(
                    arriving[m, :, at]
                )
                hidden[:, at] = value
                squares = squares + value * value
            inverse = root_mean(squares, width)
            for k in range(SIDE):
                for inner in range(PER):
                    normed = hidden[:, column(ids[1], k, inner)] * inverse
                    outs[k][at_rows, lanes(inner)] = normed.astype(jnp.bfloat16)

        each_micro(count, step)

    @pl.when(ids[0] != 0)
    def _():
        def step(m):
            at_rows = pl.ds(pl.multiple_of(m * rows, rows), rows)
            for k in range(SIDE):
                for inner in range(PER):
                    outs[k][at_rows, lanes(inner)] = cot[m, :, column(ids[1], k, inner)]

        each_micro(count, step)


def first_side_body(ids, scales, near, far, arriving, *offsets):
    count, rows, _ = arriving.shape
    start = pl.program_id(0) * count

    @pl.when(ids[0] == 0)
    def _():
        def step(m):
            i = start + m
            at_rows = pl.ds(pl.multiple_of(m * rows, rows), rows)

            def sweep(inner):
                for j in range(SIDE):
                    at = column(ids[2], j, inner)
                    hidden = f32(near[0, m, :, at]) * scale_at(
                        scales, 0, i, ids[2], j, inner
                    ) + f32(arriving[m, :, at])
                    behind = f32(far[0, m, :, at]) * scale_at(scales, 1, i, ids[2], j, inner)
                    offsets[j][at_rows, tile(inner, BLOCK)] = (hidden - behind).astype(jnp.bfloat16)

            each_micro(PER, sweep)

        each_micro(count, step)


def tile(n, size):
    return pl.ds(pl.multiple_of(n * size, size), size)


def multiply(phase, ids, read, matrix, store):
    part = matrix.shape[0] // SIDE

    @pl.when(ids[0] == phase)
    def _():
        def step(n):
            cols = tile(n, part)
            store(jnp.dot(read(), matrix[:, cols], preferred_element_type=jnp.float32), cols)

        each_micro(SIDE, step)

    @pl.when(ids[0] != phase)
    def _():
        def step(n):
            cols = tile(n, part)
            product = lax.dot_general(
                read(), matrix[cols, :], (((1,), (1,)), ((), ())), preferred_element_type=jnp.float32
            )
            store(product, cols)

        each_micro(SIDE, step)


def both(low, high):
    return jnp.concatenate([low[0], low[1], high[0], high[1]], axis=0)


def early_body(phase, ids, *refs):
    groups, matrix = refs[:6], refs[6]
    lows, highs = refs[7 : 7 + SIDE], refs[7 + SIDE :]
    for at, (outs, row) in enumerate(((lows, 0), (lows, 1), (highs, 1))):
        def store(product, cols, outs=outs, row=row):
            count = product.shape[0] // SIDE
            for k in range(SIDE):
                outs[k][row, :, cols] = product[k * count : (k + 1) * count].astype(jnp.bfloat16)

        multiply(
            phase, ids, functools.partial(both, *groups[2 * at : 2 * at + 2]), matrix, store
        )


def late_body(phase, ids, low, high, matrix, *refs):
    outs = refs[SIDE:]

    def store(product, cols):
        count = product.shape[0] // SIDE
        for k in range(SIDE):
            outs[k][0, :, cols] = product[k * count : (k + 1) * count].astype(jnp.bfloat16)

    multiply(phase, ids, functools.partial(both, low, high), matrix, store)


def add_body(ids, a0, a1, b0, b1, a_out, b_out):
    rows = a0.shape[1] // SIDE

    def step(t):
        at = (t // SIDE, tile(lax.rem(t, SIDE), rows), slice(None))
        a_out[at] = (f32(a0[at]) + f32(a1[at])).astype(jnp.bfloat16)
        b_out[at] = (f32(b0[at]) + f32(b1[at])).astype(jnp.bfloat16)

    each_micro(2 * SIDE, step)


def combine_body(phase, ids, l0, l1, l3, h0, h1, h3, o0, o1, o2, o3, v0, v1, v2, v3, peak):
    offsets, outs = (o0, o1, o2, o3), (v0, v1, v2, v3)
    count = peak.shape[0]
    rows = l0.shape[1] // count
    forward = ids[0] == phase

    def step(m):
        at = pl.ds(pl.multiple_of(m * rows, rows), rows)
        for inner in range(PER):
            cols = lanes(inner)
            best = jnp.zeros((rows, BLOCK), jnp.float32)
            for j in range(SIDE):
                terms = (l0, l1, l3) if j < 2 else (h0, h1, h3)
                value = sum(f32(term[j % 2, at, cols]) for term in terms)
                value = value + jnp.where(forward, f32(offsets[j][at, cols]), 0.0)
                outs[j][at, cols] = value.astype(jnp.bfloat16)
                best = jnp.maximum(best, jnp.abs(value))
            best = jnp.max(jnp.max(best, axis=0, keepdims=True), axis=1, keepdims=True)
            peak[m, :, cols] = jnp.broadcast_to(best, (1, BLOCK))

    each_micro(count, step)


def softened(delta, columns):
    spread = columns + epsilon
    level = delta * (code_levels / spread)
    part = level - jnp.round(level)
    square = part * part
    poly = jnp.full_like(square, SINE[-1])
    for coefficient in SINE[-2::-1]:
        poly = poly * square + coefficient
    sine = part * (0.25 - square) * poly
    smooth = level - (softness / two_pi) * sine
    return (smooth * (spread / code_levels)).astype(jnp.bfloat16)


def middle_body(ids, scales, *refs):
    own, other = refs[:SIDE], refs[SIDE : 2 * SIDE]
    own_peaks, other_peaks, between, cot = refs[2 * SIDE : 2 * SIDE + 4]
    outs = refs[2 * SIDE + 4 : 3 * SIDE + 4]
    sent, hidden, raw = refs[3 * SIDE + 4 :]
    count, rows, width = cot.shape
    start = pl.program_id(0) * count

    def step(m):
        i = start + m
        at_rows = pl.ds(pl.multiple_of(m * rows, rows), rows)

        def load(deltas, peaks, place):
            def sweep(inner):
                cols = tile(inner, BLOCK)
                for j in range(SIDE):
                    sent[m, :, column(place, j, inner)] = softened(
                        f32(deltas[j][at_rows, cols]), peaks[j, i, :, cols]
                    )

            each_micro(PER, sweep)

        def read(block, slot):
            at = lanes(block)
            return f32(between[0, m, :, at]) * (scales[slot, i, block] / code_levels) + f32(
                sent[m, :, at]
            )

        @pl.when(ids[0] == 0)
        def _():
            load(own, own_peaks, ids[2])
            for j in range(SIDE):
                for inner in range(PER):
                    raw[:, column(ids[1], j, inner)] = f32(other[j][at_rows, lanes(inner)])
            squares = jnp.zeros((rows, BLOCK), jnp.float32)
            crossed = jnp.zeros((rows, BLOCK), jnp.float32)
            for block in range(width // BLOCK):
                value = read(block, 1)
                hidden[:, lanes(block)] = value
                squares = squares + value * value
                crossed = crossed + value * raw[:, lanes(block)]
            inverse = root_mean(squares, width)
            mean = jnp.sum(crossed, axis=-1, keepdims=True) * (1.0 / width) * inverse * inverse
            for k in range(SIDE):
                for inner in range(PER):
                    at = column(ids[3], k, inner)
                    back = f32(cot[m, :, at]) + inverse * (raw[:, at] - hidden[:, at] * mean)
                    outs[k][at_rows, lanes(inner)] = back.astype(jnp.bfloat16)

        @pl.when(ids[0] != 0)
        def _():
            load(other, other_peaks, ids[1])
            squares = jnp.zeros((rows, BLOCK), jnp.float32)
            for block in range(width // BLOCK):
                value = read(block, 0)
                hidden[:, lanes(block)] = value
                squares = squares + value * value
            inverse = root_mean(squares, width)
            for k in range(SIDE):
                for inner in range(PER):
                    normed = hidden[:, column(ids[3], k, inner)] * inverse
                    outs[k][at_rows, lanes(inner)] = normed.astype(jnp.bfloat16)

    each_micro(count, step)


def middle_side_body(ids, scales, *refs):
    own, tokens = refs[:SIDE], refs[SIDE : 2 * SIDE]
    sent, near, far, cot = refs[2 * SIDE : 2 * SIDE + 4]
    offsets = refs[2 * SIDE + 4 : 3 * SIDE + 4]
    grads, hidden, raw = refs[3 * SIDE + 4 :]
    count, rows, width = cot.shape
    start = pl.program_id(0) * count

    @pl.when(ids[0] == 0)
    def _():
        def step(m):
            at_rows = pl.ds(pl.multiple_of(m * rows, rows), rows)
            for k in range(SIDE):
                for inner in range(PER):
                    at = column(ids[3], k, inner)
                    grads[m, :, at] = tokens[k][at_rows, lanes(inner)]

        each_micro(count, step)

    @pl.when(ids[0] != 0)
    def _():
        def step(m):
            i = start + m
            at_rows = pl.ds(pl.multiple_of(m * rows, rows), rows)
            for j in range(SIDE):
                for inner in range(PER):
                    raw[:, column(ids[2], j, inner)] = f32(own[j][at_rows, lanes(inner)])
            squares = jnp.zeros((rows, BLOCK), jnp.float32)
            crossed = jnp.zeros((rows, BLOCK), jnp.float32)
            for block in range(width // BLOCK):
                at = lanes(block)
                value = f32(near[0, m, :, at]) * (scales[0, i, block] / code_levels) + f32(
                    sent[m, :, at]
                )
                hidden[:, at] = value
                squares = squares + value * value
                crossed = crossed + value * raw[:, at]
            inverse = root_mean(squares, width)
            mean = jnp.sum(crossed, axis=-1, keepdims=True) * (1.0 / width) * inverse * inverse
            for block in range(width // BLOCK):
                at = lanes(block)
                back = f32(cot[m, :, at]) + inverse * (raw[:, at] - hidden[:, at] * mean)
                grads[m, :, at] = back.astype(jnp.bfloat16)

            def sweep(inner):
                for j in range(SIDE):
                    at = column(ids[4], j, inner)
                    behind = f32(far[0, m, :, at]) * scale_at(scales, 1, i, ids[4], j, inner)
                    offsets[j][at_rows, tile(inner, BLOCK)] = (hidden[:, at] - behind).astype(
                        jnp.bfloat16
                    )

            each_micro(PER, sweep)

        each_micro(count, step)


def last_body(ids, scales, r0, r1, r2, r3, peaks, near, arriving, upstream, sent, outs, grads, hidden, raw):
    result = (r0, r1, r2, r3)
    count, rows, width = arriving.shape
    start = pl.program_id(0) * count
    b = ids[4]

    @pl.when(ids[0] == 0)
    def _():
        def step(m):
            at_rows = pl.ds(pl.multiple_of(m * rows, rows), rows)
            for j in range(SIDE):
                for inner in range(PER):
                    raw[:, column(b, j, inner)] = f32(result[j][at_rows, lanes(inner)])
            squares = jnp.zeros((rows, BLOCK), jnp.float32)
            crossed = jnp.zeros((rows, BLOCK), jnp.float32)
            for block in range(width // BLOCK):
                at = lanes(block)
                value = f32(near[0, m, :, at]) * (
                    scales[0, start + m, block] / code_levels
                ) + f32(arriving[m, :, at])
                hidden[:, at] = value
                squares = squares + value * value
                crossed = crossed + value * raw[:, at]
            inverse = root_mean(squares, width)
            mean = jnp.sum(crossed, axis=-1, keepdims=True) * (1.0 / width) * inverse
            for block in range(width // BLOCK):
                at = lanes(block)
                unrounded = hidden[:, at] * inverse
                back = f32(upstream[m, :, at]) + inverse * (raw[:, at] - unrounded * mean)
                grads[m, :, at] = back.astype(jnp.bfloat16)

        each_micro(count, step)
        outs[...] = sent[...]

    @pl.when(ids[0] != 0)
    def _():
        def step(m):
            at_rows = pl.ds(pl.multiple_of(m * rows, rows), rows)

            def sweep(inner):
                for j in range(SIDE):
                    outs[m, :, column(b, j, inner)] = softened(
                        f32(result[j][at_rows, tile(inner, BLOCK)]),
                        peaks[j, start + m, :, tile(inner, BLOCK)],
                    )

            each_micro(PER, sweep)

        each_micro(count, step)
        grads[...] = upstream[...]


def turn_body(ids, *refs):
    groups, out = refs[: 2 * SIDE], refs[-1]
    rows = groups[0].shape[1]
    for half in range(2):
        for j in range(SIDE):
            def step(i):
                out[:, tile((2 * half + i) * SIDE + j, rows)] = groups[2 * j + half][i].T

            each_micro(2, step)


def gradient_body(ids, left, *refs):
    groups, outs, result = refs[: 2 * SIDE], refs[2 * SIDE : -1], refs[-1]
    span = left.shape[0]
    part = span // SIDE
    depth = left.shape[1] // SIDE

    def product(rows, columns):
        total = None
        for i in range(SIDE):
            right = jnp.concatenate(
                [groups[2 * i + j // 2][j % 2, :, columns] for j in range(SIDE)], axis=0
            )
            term = jnp.dot(
                left[rows, i * depth : (i + 1) * depth], right, preferred_element_type=jnp.float32
            )
            total = term if total is None else total + term
        return total.astype(jnp.bfloat16)

    def places(t):
        k, n = t // SIDE, lax.rem(t, SIDE)
        return k, tile(n, part), tile(lax.rem(ids[5] + k, SIDE), part)

    @pl.when(ids[0] == 0)
    def _():
        def step(t):
            k, each, mine = places(t)
            result[k, each, :] = product(each, mine)

        each_micro(SIDE * SIDE, step)

    @pl.when(ids[0] != 0)
    def _():
        def step(t):
            k, each, mine = places(t)
            result[k, each, :] = product(mine, each).T

        each_micro(SIDE * SIDE, step)

    for k in range(SIDE):
        outs[k][...] = result[k]


def total_body(ids, q0, q1, q2, q3, *outs):
    part = q0.shape[1]
    for k in range(SIDE):
        at = tile(lax.rem(ids[6] + k, SIDE), part)
        total = (f32(q0[at, :]) + f32(q1[at, :])) + (f32(q2[at, :]) + f32(q3[at, :]))
        outs[k][...] = total.astype(jnp.bfloat16)


def choose_body(ids, r0, r1, r2, r3, *outs):
    for l in range(SIDE):
        k = lax.rem(ids[6] - ids[5] - l + 2 * SIDE, SIDE)
        for at, source in enumerate((r0, r1, r2, r3)):
            @pl.when(k == at)
            def _():
                outs[l][...] = source[...]


def pass_body(ids, *refs):
    half = len(refs) // 2
    for source, target in zip(refs[:half], refs[half:]):
        target[...] = source[...]


def assemble_body(ids, a0, b0, a1, b1, out):
    depth = a0.shape[1]
    odd = lax.rem(ids[5], 2)
    for k in range(SIDE):
        row = lax.rem(ids[6] - k + SIDE, SIDE) * SIDE
        for at, group in ((2 * odd, a0), (2 * odd + 1, b0), (2 - 2 * odd, a1), (3 - 2 * odd, b1)):
            out[tile(row + at, depth), :] = group[k]


def finish_body(ids, f0, f1, f2, f3, out):
    part = f0.shape[1]
    for l, piece in enumerate((f0, f1, f2, f3)):
        out[:, tile(lax.rem(ids[5] - l + SIDE, SIDE), part)] = f32(piece[...])


def local(in_delta, weight, cache_codes, cache_scales, cotangent):
    s = lax.axis_index(SECTION)
    z = lax.axis_index("tensor_0")
    y = lax.axis_index(FAST)
    x = lax.axis_index(DP)
    micro_count, local_rows, width = in_delta.shape
    span = width // SIDE
    bf16, single = jnp.bfloat16, jnp.float32
    here = jnp.where(s == 0, z, y)
    there = jnp.where(s == 0, y, z)
    ids = jnp.stack([s, here, there, there, here, x, y]).astype(jnp.int32)

    count = micro_count // STEPS
    rows = micro_count * local_rows
    grid = (STEPS,)
    flat = (count, local_rows, width)
    in_smem = pl.BlockSpec(memory_space=pltpu.SMEM)
    piece = pl.BlockSpec((count * local_rows, span), lambda i, ids: (i, 0))
    piece_shape = jax.ShapeDtypeStruct((rows, span), bf16)
    whole = pl.BlockSpec(flat, lambda i, ids: (i, 0, 0))
    whole_shape = jax.ShapeDtypeStruct((micro_count, local_rows, width), bf16)
    work = [pltpu.VMEM((local_rows, width), single)]
    peak_shape = (micro_count, 1, span)
    peaks_spec = pl.BlockSpec((SIDE, *peak_shape), lambda i, ids: (0, 0, 0, 0))
    half = pl.BlockSpec((2, rows, span), lambda i, ids: (0, 0, 0))
    full_piece = pl.BlockSpec((rows, span), lambda i, ids: (0, 0))
    square = pl.BlockSpec((span, span), lambda i, ids: (0, 0))
    half_shape = jax.ShapeDtypeStruct((2, rows, span), bf16)
    codes, scales = cache_codes[0], cache_scales[0, :, :, 0, :]
    near = pl.BlockSpec((1, *flat), lambda i, ids: (0, i, 0, 0))
    far = pl.BlockSpec((1, *flat), lambda i, ids: (1, i, 0, 0))
    between = pl.BlockSpec((1, *flat), lambda i, ids: (1 - ids[0], i, 0, 0))

    depth = weight.shape[1] // 2

    def corner(k):
        return pl.BlockSpec(
            (depth, span), lambda i, ids: (lax.rem(ids[5], 2), lax.rem(ids[6] + k, SIDE))
        )

    halves = call(
        pass_body,
        ids,
        (1,),
        [weight[0]] * SIDE,
        [corner(k) for k in range(SIDE)],
        [jax.ShapeDtypeStruct((depth, span), bf16)] * SIDE,
        [pl.BlockSpec((depth, span), lambda i, ids: (0, 0))] * SIDE,
    )
    halves = [halves[0]] + [ring(halves[k], FAST, k) for k in (1, 2, 3)]
    upper = jnp.stack([part[: depth // 2] for part in halves])
    lower = jnp.stack([part[depth // 2 :] for part in halves])
    block = call(
        assemble_body,
        ids,
        (1,),
        [upper, lower, ring(upper, DP, 1), ring(lower, DP, -1)],
        [pl.BlockSpec((SIDE, depth // 2, span), lambda i, ids: (0, 0, 0))] * SIDE,
        jax.ShapeDtypeStruct((span, span), bf16),
        square,
    )

    def spread_out(pieces, phase):
        arrived = [pieces[0]] + [shift(pieces[k], phase, ROWS, k) for k in (1, 2, 3)]
        low, high = jnp.stack(arrived[:2]), jnp.stack(arrived[2:])
        after = [shift(low, phase, COLUMNS, 1)]
        before = [shift(high, phase, COLUMNS, -1)]
        after.append(shift(high, phase, COLUMNS, 1))
        before.insert(0, shift(low, phase, COLUMNS, -1))
        across = [shift(after[0], phase, COLUMNS, 1), shift(before[1], phase, COLUMNS, -1)]
        return [low, high, *after, *across, *before]

    def moved(offsets, phase):
        return [offsets[0]] + [shift(offsets[j], phase, COLUMNS, j) for j in (1, 2, 3)]

    def products(groups, phase):
        made = call(
            functools.partial(early_body, phase),
            ids,
            (1,),
            [*groups[:4], *groups[6:], block],
            [half] * 6 + [square],
            [half_shape] * (2 * SIDE),
            [half] * (2 * SIDE),
            flops=6 * SIDE * rows * span * span,
        )
        lows, highs = made[:SIDE], made[SIDE:]

        def sent(value, steps):
            return shift(value, phase, ROWS, steps)

        opposite_low = sent(lows[2], -1)
        last_low = sent(lows[3], 1)
        late = pl.BlockSpec((1, rows, span), lambda i, ids: (0, 0, 0))
        highs = call(
            functools.partial(late_body, phase),
            ids,
            (1,),
            [*groups[4:6], block, *highs],
            [half, half, square] + [pl.BlockSpec(memory_space=pl.ANY)] * SIDE,
            [half_shape] * SIDE,
            [late] * SIDE,
            flops=2 * SIDE * rows * span * span,
            aliases={4 + k: k for k in range(SIDE)},
        )
        opposite_high = sent(highs[2], 1)
        first_high = sent(highs[1], -1)
        first_low, last_high = call(
            add_body,
            ids,
            (1,),
            [lows[1], opposite_low, highs[3], opposite_high],
            [half] * 4,
            [half_shape] * 2,
            [half] * 2,
        )
        first_low = sent(first_low, -1)
        last_high = sent(last_high, 1)
        return [lows[0], first_low, last_low, highs[0], first_high, last_high]

    def returned(arrived, offsets, phase):
        *sent, peak = call(
            functools.partial(combine_body, phase),
            ids,
            (1,),
            [*arrived, *offsets],
            [half] * 6 + [full_piece] * SIDE,
            [piece_shape] * SIDE + [jax.ShapeDtypeStruct(peak_shape, single)],
            [full_piece] * SIDE + [pl.BlockSpec(peak_shape, lambda i, ids: (0, 0, 0))],
        )
        for k, other in [(k, shift(peak, phase, ROWS, k)) for k in (1, 2, 3)]:
            peak = jnp.maximum(peak, other)
        home = [sent[0]] + [shift(sent[j], phase, COLUMNS, -j) for j in (1, 2, 3)]
        peaks = jnp.stack([peak] + [shift(peak, phase, COLUMNS, -j) for j in (1, 2, 3)])
        return home, peaks

    tokens = call(
        first_body,
        ids,
        grid,
        [scales, codes, in_delta, cotangent],
        [in_smem, near, whole, whole],
        [piece_shape] * SIDE,
        [piece] * SIDE,
        work,
    )
    groups = spread_out(tokens, 0)
    offsets = call(
        first_side_body,
        ids,
        grid,
        [scales, codes, codes, in_delta],
        [in_smem, near, far, whole],
        [piece_shape] * SIDE,
        [piece] * SIDE,
    )
    offsets = moved(offsets, 0)
    own, own_peaks = returned(products(groups, 0), offsets, 0)
    other_peaks = crossed_over(own_peaks)
    other = [crossed_over(own[j]) for j in range(SIDE)]
    *tokens, sent = call(
        middle_body,
        ids,
        grid,
        [scales, *own, *other, own_peaks, other_peaks, codes, cotangent],
        [in_smem] + [piece] * (2 * SIDE) + [peaks_spec, peaks_spec, between, whole],
        [piece_shape] * SIDE + [whole_shape],
        [piece] * SIDE + [whole],
        work * 2,
    )
    groups_next = spread_out(tokens, 1)
    *offsets, upstream = call(
        middle_side_body,
        ids,
        grid,
        [scales, *own, *tokens, sent, codes, codes, cotangent],
        [in_smem] + [piece] * (2 * SIDE) + [whole, near, far, whole],
        [piece_shape] * SIDE + [whole_shape],
        [piece] * SIDE + [whole],
        work * 2,
    )
    offsets = moved(offsets, 1)
    result, peaks = returned(products(groups_next, 1), offsets, 1)
    outs, grads = call(
        last_body,
        ids,
        grid,
        [scales, *result, peaks, codes, in_delta, upstream, sent],
        [in_smem] + [piece] * SIDE + [peaks_spec, near, whole, whole, whole],
        [whole_shape, whole_shape],
        [whole, whole],
        work * 2,
    )

    total_rows = SIDE * SIDE * rows
    part = span // SIDE
    gathered_specs = [half] * (2 * SIDE)
    tall = pl.BlockSpec((span, part), lambda i, ids: (0, 0))
    small = pl.BlockSpec((part, part), lambda i, ids: (0, 0))
    flipped = pl.BlockSpec((span, total_rows), lambda i, ids: (0, 0))
    left = call(
        turn_body,
        ids,
        (1,),
        groups,
        gathered_specs,
        jax.ShapeDtypeStruct((span, total_rows), bf16),
        flipped,
    )
    partials = call(
        gradient_body,
        ids,
        (1,),
        [left, *groups_next],
        [flipped, *gathered_specs],
        [jax.ShapeDtypeStruct((span, part), bf16)] * SIDE,
        [tall] * SIDE,
        [pltpu.VMEM((SIDE, span, part), bf16)],
        flops=2 * total_rows * span * span,
    )
    arrived = [partials[0]] + [ring(partials[k], DP, k) for k in (1, 2, 3)]
    pieces = call(
        total_body,
        ids,
        (1,),
        arrived,
        [tall] * SIDE,
        [jax.ShapeDtypeStruct((part, part), bf16)] * SIDE,
        [small] * SIDE,
    )
    pieces = [pieces[0]] + [ring(pieces[k], FAST, k) for k in (1, 2, 3)]
    pieces = call(
        choose_body,
        ids,
        (1,),
        pieces,
        [small] * SIDE,
        [jax.ShapeDtypeStruct((part, part), bf16)] * SIDE,
        [small] * SIDE,
    )
    pieces = [pieces[0]] + [ring(pieces[k], DP, k) for k in (1, 2, 3)]
    weight_grad = call(
        finish_body,
        ids,
        (1,),
        pieces,
        [small] * SIDE,
        jax.ShapeDtypeStruct((part, span), single),
        pl.BlockSpec((part, span), lambda i, ids: (0, 0)),
    )
    return outs[None], grads[None], weight_grad[None]


def solution(mesh):
    finer = Mesh(
        mesh.devices.reshape(mesh.shape[DP], mesh.shape[SECTION], SIDE, SIDE),
        (DP, SECTION, "tensor_0", FAST),
    )
    return jax.shard_map(
        local,
        mesh=finer,
        in_specs=(
            P(None, DP_TENSOR, None),
            P(SECTION, TENSOR, None),
            P(SECTION, None, None, DP_TENSOR, None),
            P(SECTION, None, None, DP, None),
            P(None, DP_TENSOR, None),
        ),
        out_specs=(
            P(SECTION, None, DP_TENSOR, None),
            P(SECTION, None, DP_TENSOR, None),
            P(SECTION, TENSOR, DP),
        ),
        check_vma=False,
    )
```
